32 devices in a mesh: groups: 2 (over y), adapter: 4 (over x, core), tensor: 4 (over z).
Axes of the slice: x: 2, y: 2, z: 4, core: 2. Of those that a mesh axis runs over, the one named last changes fastest.
Arguments:
- tokens: bfloat16 [2048, 8192], P(('groups', 'adapter'), 'tensor'), parts along dimension 0, may hold values from -6 to 6
- query_weight: bfloat16 [8192, 8192], P('tensor', 'adapter'), may hold values from -0.0625 to 0.0625
- adapter_down_weight: bfloat16 [128, 16, 8192], P('adapter', None, 'tensor'), may hold values from -0.0625 to 0.0625
- adapter_up_weight: bfloat16 [128, 16, 8192], P('adapter'), may hold values from -1.5 to 1.5
- block_adapter_ids: int32 [16], P('groups'), parts along dimension 0, may hold values from 0 to 127, as said below
- block_live_count: int32 [16], P('groups'), parts along dimension 0, may hold values from 1 to 128
- adapter_slot_index: int32 [256], P('groups'), parts along dimension 0, may hold values from 0 to 127, as said below
Outputs:
- query: bfloat16 [2048, 8192], P(('groups', 'tensor'), 'adapter'), parts along dimension 0
The draws below stay inside these ranges and needn't reach their ends.
There are 2 independent parts, one for each index of `groups`. The reference program is written for one: setup_inputs(seed, part) draws one part's arguments, and reference() takes and returns one part's arrays. A program takes and returns all parts, laid end to end along the dimension named above; an argument that names none is the same for every part. Nothing has to cross between parts.
Inputs may be any that keep to these rules, and one draw needn't show every extreme that they name: Counting blocks by the owner range adapter_slot_index[block_adapter_ids[k]] // 32, no owner has more than 4 blocks, and one owner has exactly 4 in every draw. `adapter_slot_index`: A permutation: each slot holds exactly one adapter.
All inputs are finite; a program needn't handle non-finite values.
Results may differ from the reference program's by a relative error of at most 0.014.
Values may be sent and summed in bfloat16 or wider, within the bound.
A program may use at most 128 MiB of HBM per device.

```python
import jax
import jax.numpy as jnp

MODEL_WIDTH = 8192
QUERY_OUTPUTS = 8192
ADAPTER_RANK = 16
ADP_DEV = 32
BLOCK = 128
ADAPTER_COUNT = 128
FEAT = 2048
CAP = 4
BLOCKS = 8
TOKENS = 1024


def plan_draw(key):
    owner_count = ADAPTER_COUNT // ADP_DEV
    slot_table = jax.random.permutation(jax.random.fold_in(key, 101), jnp.arange(ADAPTER_COUNT, dtype=jnp.int32)).astype(jnp.int32)
    holder = jnp.argsort(slot_table, stable=True).astype(jnp.int32)
    hottest = jax.random.randint(jax.random.fold_in(key, 102), (), 0, owner_count, dtype=jnp.int32)
    seat_owner = jnp.arange((owner_count - 1) * CAP, dtype=jnp.int32) // CAP
    seat_owner = seat_owner + (seat_owner >= hottest).astype(jnp.int32)
    seat_owner = jax.random.permutation(jax.random.fold_in(key, 103), seat_owner)[:BLOCKS - CAP]
    owner_list = jnp.concatenate([jnp.full((CAP,), hottest, jnp.int32), seat_owner.astype(jnp.int32)])
    owner_list = jax.random.permutation(jax.random.fold_in(key, 104), owner_list)
    local_slot = jax.random.randint(jax.random.fold_in(key, 105), (BLOCKS,), 0, ADP_DEV, dtype=jnp.int32)
    adapters = holder[owner_list * ADP_DEV + local_slot]
    return (slot_table, adapters.astype(jnp.int32))


def draw_block_adapter_ids(key, part):
    return plan_draw(key)[1]


def draw_adapter_slot_index(key, part):
    return plan_draw(key)[0]


def touch_ends(drawn, stream_key, low, top_value):
    longest = drawn.shape.index(max(drawn.shape))
    spots = []
    for shift in (0, 1):
        where = [jax.random.randint(jax.random.fold_in(stream_key, axis), (), 0, length) for axis, length in enumerate(drawn.shape)]
        where[longest] = (where[longest] + shift) % drawn.shape[longest]
        spots.append(tuple(where))
    return drawn.at[spots[0]].set(low).at[spots[1]].set(top_value)


def levels(own_key, dims, cuts, low, largest):
    def one(position, blocks):
        draws = jax.random.uniform(jax.random.fold_in(jax.random.fold_in(own_key, 6), position), (blocks,), jnp.float32, low / len(cuts), largest / len(cuts))
        return jnp.repeat(jnp.exp(draws), dims[position] // blocks).reshape((-1,) + (1,) * (len(dims) - position - 1))

    factor_of = one(*cuts[0])
    for cut in cuts[1:]:
        factor_of = factor_of * one(*cut)
    return factor_of


def normal_values(rng, extent, spread, reach, pieces=(), held_as=jnp.bfloat16):
    array = spread * jax.random.normal(rng, extent, jnp.float32)
    if pieces:
        array = array * levels(rng, extent, pieces, -0.22, 0.18)
    return jnp.clip(array, -reach, reach).astype(held_as)


def setup_inputs(seed: int = 0, part: int = 0) -> dict:
    key_list = jax.random.split(jax.random.key(seed), 8)
    own_keys = jax.random.split(jax.random.fold_in(key_list[7], part), 8)
    tokens = normal_values(own_keys[0], (TOKENS, MODEL_WIDTH), 1.0, 6.0, ((0, 4), (1, 4)))
    query_weight = normal_values(key_list[1], (MODEL_WIDTH, QUERY_OUTPUTS), MODEL_WIDTH ** -0.5, 0.0625, ((0, 4), (1, 4)))
    adapter_down_weight = normal_values(key_list[2], (ADAPTER_COUNT, ADAPTER_RANK, MODEL_WIDTH), MODEL_WIDTH ** -0.5, 0.0625, ((0, 4), (2, 4)))
    adapter_up_weight = normal_values(key_list[3], (ADAPTER_COUNT, ADAPTER_RANK, QUERY_OUTPUTS), ADAPTER_RANK ** -0.5, 1.5, ((0, 4),))
    block_adapter_ids = draw_block_adapter_ids(jax.random.fold_in(jax.random.fold_in(key_list[7], part), 71), part)
    block_live_count = touch_ends(jax.random.randint(own_keys[5], (BLOCKS,), 1, BLOCK + 1), jax.random.fold_in(own_keys[5], 1), 1, BLOCK).astype(jnp.int32)
    adapter_slot_index = draw_adapter_slot_index(jax.random.fold_in(jax.random.fold_in(key_list[7], part), 71), part)
    return dict(tokens=tokens, query_weight=query_weight, adapter_down_weight=adapter_down_weight, adapter_up_weight=adapter_up_weight, block_adapter_ids=block_adapter_ids, block_live_count=block_live_count, adapter_slot_index=adapter_slot_index)


def reference(tokens, query_weight, adapter_down_weight, adapter_up_weight, block_adapter_ids, block_live_count, adapter_slot_index):
    block_slot_index = adapter_slot_index[block_adapter_ids].astype(jnp.int32)
    down_weight_blocks = adapter_down_weight[block_slot_index].astype(jnp.float32)
    up_weight_blocks = adapter_up_weight[block_slot_index].astype(jnp.float32)
    positions = jnp.arange(BLOCK, dtype=jnp.int32)
    live_mask = (positions[None, :] < block_live_count[:, None]).astype(jnp.float32)
    token_blocks = tokens.reshape(BLOCKS, BLOCK, MODEL_WIDTH).astype(jnp.float32)
    total = jnp.zeros((TOKENS, QUERY_OUTPUTS), jnp.float32)
    for slice_index in range(MODEL_WIDTH // FEAT):
        low_edge = slice_index * FEAT
        high_edge = low_edge + FEAT
        shrunk = jnp.einsum("ksd,krd->ksr", token_blocks[:, :, low_edge:high_edge], down_weight_blocks[:, :, low_edge:high_edge])
        shrunk = (shrunk * live_mask[:, :, None]).astype(jnp.bfloat16)
        adapter_part = jnp.einsum("ksr,krf->ksf", shrunk.astype(jnp.float32), up_weight_blocks).reshape(TOKENS, QUERY_OUTPUTS)
        base_part = jnp.dot(tokens[:, low_edge:high_edge], query_weight[low_edge:high_edge, :], preferred_element_type=jnp.float32)
        partial_value = (base_part + 2.0 * adapter_part).astype(jnp.bfloat16)
        total = total + partial_value.astype(jnp.float32)
    return total.astype(jnp.bfloat16)
```

```python
import functools

import jax
import jax.numpy as jnp
from jax import lax
from jax.experimental import pallas as pl
from jax.experimental.pallas import tpu as pltpu
from jax.sharding import PartitionSpec as P

BLOCK = 128
SCALE = 2.0
MESH = pl.DeviceIdType.MESH
PRE = 2


def kernel(
    A, T,
    ids, live, slots, tok_hbm, w_hbm, dn_hbm, up_hbm, out_ref,
    tok, w, dn, up, buf, acc, dn_send, dn_recv, up_send, up_recv, s_send, s_recv,
    tok_sem, ld_sem, w_sem, par_ss, par_rs, x_ss, x_rs, f_ss, f_rs,
    dn_ss, dn_rs, up_ss, up_rs, s_ss, s_rs, fl_ss, fl_rs, ready,
):
    a = lax.axis_index("adapter")
    t = lax.axis_index("tensor")
    chips = A // 2
    x, core = a // 2, a % 2
    partner = 2 * x + 1 - core
    nb = tok.shape[0]
    nb_a, nb_t = nb // A, nb // T
    half = BLOCK // 2
    per_dev = dn_hbm.shape[0]
    np_, _, cp = w.shape
    cols = np_ * cp
    steps = (T - 1) * nb_t
    near = chips == 2 and nb_a == nb_t
    pre_n = min(PRE, np_) if near else 0

    def tok_load(b):
        return pltpu.make_async_copy(
            tok_hbm.at[pl.ds(b * BLOCK, BLOCK)], tok.at[a * nb_a + b], tok_sem.at[b]
        )

    def w_load(p):
        c = pl.ds(pl.multiple_of(p * cp, cp), cp)
        return pltpu.make_async_copy(w_hbm.at[:, c], w.at[p], w_sem.at[p])

    dn_load = pltpu.make_async_copy(dn_hbm, dn, ld_sem.at[0])
    up_load = pltpu.make_async_copy(up_hbm, up, ld_sem.at[1])

    tok_load(0).start()
    w_load(0).start()
    for b in range(1, nb_a):
        tok_load(b).start()
    for p in range(1, np_):
        w_load(p).start()
    dn_load.start()
    up_load.start()

    barrier = pltpu.get_barrier_semaphore()

    def greet(**to):
        pl.semaphore_signal(barrier, inc=1, device_id=to, device_id_type=MESH)

    @pl.when(t > 0)
    def _():
        greet(tensor=t - 1)

    @pl.when(t < T - 1)
    def _():
        greet(tensor=t + 1)

    for i in range(1, A):
        greet(adapter=(a + i) % A)

    if near:
        lead_r = jnp.where(a >= 1, a, 1)
        lead_l = jnp.where(a <= T - 2, a, T - 2)
        first_r = (T - 1 - lead_r) * nb_t
        first_l = lead_l * nb_t
        pre = jnp.logical_or(
            jnp.logical_and(t == 0, a >= 1), jnp.logical_and(t == T - 1, a <= T - 2)
        )
    else:
        first_r = first_l = 0

    def place(way, k):
        first = first_l if way else first_r
        m = jnp.where(k - 1 < first, k - 1, k)
        m = jnp.where(k == 0, first, m)
        d = m // nb_t
        return (d if way else T - 1 - d), m % nb_t

    def flow(way, to, slot, h, p):
        return pltpu.make_async_remote_copy(
            buf.at[way, slot, h, p], buf.at[way, slot, h, p],
            fl_ss.at[way, slot, h, p], fl_rs.at[way, slot, h, p],
            device_id={"tensor": to}, device_id_type=MESH,
        )

    right, left = (t + 1) % T, (t + T - 1) % T

    def toward(way, slot, h, p):
        return flow(way, left if way else right, slot, h, p)

    def base(q, p):
        return jnp.dot(tok[q], w[p], preferred_element_type=jnp.float32)

    if near:
        pre_way = jnp.where(t == 0, 0, 1)
        pre_slot = jnp.where(t == 0, jnp.maximum(a - 1, 0), jnp.minimum(a, T - 2))
        pre_to = jnp.where(t == 0, 1, T - 2)

    tok_load(0).wait()
    if pre_n:

        @pl.when(pre)
        def _():
            def one(p, _):
                w_load(p).wait()
                buf[pre_way, pre_slot, 0, p] = base(a * nb_a, p).astype(buf.dtype)
                return 0

            lax.fori_loop(0, pre_n, one, 0)

    for b in range(1, nb_a):
        tok_load(b).wait()

    ends = jnp.where(t > 0, 1, 0) + jnp.where(t < T - 1, 1, 0)
    pl.semaphore_wait(barrier, A - 1 + ends)

    if pre_n:

        @pl.when(pre)
        def _():
            for p in range(pre_n):
                flow(pre_way, pre_to, pre_slot, 0, p).start()

    def par_copy(b):
        r = tok.at[a * nb_a + b]
        return pltpu.make_async_remote_copy(
            r, r, par_ss.at[b], par_rs.at[b], device_id={"adapter": partner}, device_id_type=MESH
        )

    def lead_core(c):
        return jnp.where(2 * c >= chips, 1, 0)

    def row_block(c, m):
        k = jnp.where(m < nb_a, lead_core(c), 1 - lead_core(c))
        return (2 * c + k) * nb_a + m % nb_a, k

    def part(q, k):
        return tok.at[q, pl.ds(pl.multiple_of(k * half, half), half)]

    def x_copy(i, m):
        r = part(row_block(x, m)[0], core)
        return pltpu.make_async_remote_copy(
            r, r, x_ss.at[i, m], x_rs.at[x, m],
            device_id={"adapter": 2 * ((x + i) % chips) + core}, device_id_type=MESH,
        )

    def x_arrival(c, m):
        r = part(row_block(c, m)[0], core)
        return pltpu.make_async_remote_copy(
            r, r, x_ss.at[0, m], x_rs.at[c, m],
            device_id={"adapter": partner}, device_id_type=MESH,
        )

    def pass_on(c, m):
        r = part(row_block(c, m)[0], core)
        return pltpu.make_async_remote_copy(
            r, r, f_ss.at[c, m], f_rs.at[c, m],
            device_id={"adapter": partner}, device_id_type=MESH,
        )

    for b in range(nb_a):
        par_copy(b).start()
    for m in range(2 * nb_a):

        @pl.when(row_block(x, m)[1] != core)
        def _():
            par_copy(m % nb_a).wait_recv()

        for i in range(1, chips):
            x_copy(i, m).start()

    def fetch(c, m):
        x_arrival(c, m).wait_recv()
        pass_on(c, m).start()

    def fetched(c, m):
        pass_on(c, m).wait_recv()

    def tell(i, to):
        pl.semaphore_signal(ready.at[i], inc=1, device_id={"tensor": to}, device_id_type=MESH)

    @pl.when(t == 0)
    def _():
        tell(0, right)

    @pl.when(t == T - 1)
    def _():
        tell(1, left)

    def relay():
        @pl.when(jnp.logical_and(t > 0, t < T - 1))
        def _():
            pl.semaphore_wait(ready.at[0], 1)
            tell(0, right)
            pl.semaphore_wait(ready.at[1], 1)
            tell(1, left)

    def all_in():
        @pl.when(t == 0)
        def _():
            pl.semaphore_wait(ready.at[1], 1)

        @pl.when(t == T - 1)
        def _():
            pl.semaphore_wait(ready.at[0], 1)

    def slot_of(k):
        return slots[ids[k]]

    def dn_copy(i):
        to = (a + i) % A
        return pltpu.make_async_remote_copy(
            dn_send.at[to], dn_recv.at[a], dn_ss.at[i], dn_rs.at[i],
            device_id={"adapter": to}, device_id_type=MESH,
        )

    def up_copy(i):
        to = (a + i) % A
        return pltpu.make_async_remote_copy(
            up_send.at[to], up_recv.at[a], up_ss.at[i], up_rs.at[i],
            device_id={"adapter": to}, device_id_type=MESH,
        )

    def s_dest(b):
        k = a * nb_a + b
        return k // nb_t, k % nb_t

    def s_copy(i, b):
        d, kk = s_dest(b)
        return pltpu.make_async_remote_copy(
            s_send.at[b], s_recv.at[t, kk], s_ss.at[i, b], s_rs.at[t, kk],
            device_id={"adapter": (a + i) % A, "tensor": d}, device_id_type=MESH,
        )

    def send_adapters():
        dn_load.wait()
        for i in range(A):
            for b in range(nb_a):
                dn_send[i, b] = dn[lax.rem(slot_of(i * nb_a + b), per_dev)]
        dn_recv[a] = dn_send[a]
        for i in range(1, A):
            dn_copy(i).start()
        up_load.wait()
        for b in range(nb_t):
            sl = lax.rem(slot_of(t * nb_t + b), per_dev)
            for i in range(A):
                up_send[i, b] = up[sl, :, i * cols:(i + 1) * cols]
        up_recv[a] = up_send[a]
        for i in range(1, A):
            up_copy(i).start()

    def send_shrunk():
        all_in()
        for i in range(1, A):
            dn_copy(i).wait_recv()
        for b in range(nb_a):
            k = a * nb_a + b
            mine = dn_recv[lax.div(slot_of(k), per_dev), b]
            s = lax.dot_general(
                mine, tok[k], (((1,), (1,)), ((), ())), preferred_element_type=jnp.float32
            )
            keep = lax.broadcasted_iota(jnp.int32, s.shape, 1) < live[k]
            s_send[b] = jnp.where(keep, s, 0.0).astype(s_send.dtype)
            d, kk = s_dest(b)
            for i in range(A):
                if i:
                    s_copy(i, b).start()
                else:
                    @pl.when(d == t)
                    def _():
                        s_recv[t, kk] = s_send[b]

                    @pl.when(d != t)
                    def _():
                        s_copy(0, b).start()

    def wait_adapters():
        for i in range(1, A):
            up_copy(i).wait_recv()
        for b in range(nb_t):
            owner = (t * nb_t + b) // nb_a
            for tt in range(T):
                c = pltpu.make_async_remote_copy(
                    s_send.at[0], s_recv.at[tt, b], s_ss.at[0, 0], s_rs.at[tt, b],
                    device_id={"adapter": partner}, device_id_type=MESH,
                )

                @pl.when(jnp.logical_or(owner != a, t != tt))
                def _():
                    c.wait_recv()

    remote = [(i, m) for i in range(1, chips) for m in range(2 * nb_a)]
    if not near:
        for i, m in remote:
            fetch((x + i) % chips, m)
        for i, m in remote:
            fetched((x + i) % chips, m)

    def advance(way, k, p):
        d, h = place(way, k)
        slot = d if way else d - 1
        q = d * nb_t + h
        go = (d < t) if way else (d > t)
        if pre_n:
            done = jnp.logical_and(jnp.logical_and(pre, k == 0), p < pre_n)
            go = jnp.logical_and(go, jnp.logical_not(done))

        @pl.when(go)
        def _():
            mine = base(q, p)
            fresh = (t == T - 1) if way else (t == 0)

            @pl.when(fresh)
            def _():
                buf[way, slot, h, p] = mine.astype(buf.dtype)

            @pl.when(jnp.logical_not(fresh))
            def _():
                toward(way, slot, h, p).wait_recv()
                buf[way, slot, h, p] = (
                    mine + buf[way, slot, h, p].astype(jnp.float32)
                ).astype(buf.dtype)

            toward(way, slot, h, p).start()

    def step(k, _):
        if near:

            @pl.when(jnp.logical_and(k >= 1, k <= 2 * nb_a))
            def _():
                fetch(1 - x, k - 1)
                fetched(1 - x, k - 1)

        @pl.when(k == min(1, steps - 1))
        def _():
            relay()

        @pl.when(k == min(2, steps - 1))
        def _():
            send_adapters()

        @pl.when(k == max(steps - 2, 0))
        def _():
            send_shrunk()

        def panel(p, _):
            loaded = k == 0
            if pre_n:
                loaded = jnp.logical_and(
                    loaded, jnp.logical_not(jnp.logical_and(pre, p < pre_n))
                )

            @pl.when(loaded)
            def _():
                w_load(p).wait()

            advance(0, k, p)
            advance(1, k, p)
            h = k - (steps - nb_t)

            @pl.when(h >= 0)
            def _():
                acc[h, p] = base(t * nb_t + h, p)

            return 0

        lax.fori_loop(0, np_, panel, 0)
        return 0

    lax.fori_loop(0, steps, step, 0)
    wait_adapters()

    def last(n, _):
        h, p = n // np_, n % np_
        own = lax.div(slot_of(t * nb_t + h), per_dev)
        u = up_recv[own, h, :, pl.ds(pl.multiple_of(p * cp, cp), cp)]
        lhs = s_recv[:, h].reshape(T * s_recv.shape[2], BLOCK)
        acc[h, p] = acc[h, p] + SCALE * lax.dot_general(
            lhs, jnp.concatenate([u] * T, axis=0), (((0,), (0,)), ((), ())),
            preferred_element_type=jnp.float32,
        )

        @pl.when(t > 0)
        def _():
            slot = jnp.maximum(t - 1, 0)
            toward(0, slot, h, p).wait_recv()
            acc[h, p] = acc[h, p] + buf[0, slot, h, p].astype(jnp.float32)

        @pl.when(t < T - 1)
        def _():
            slot = jnp.minimum(t, T - 2)
            toward(1, slot, h, p).wait_recv()
            acc[h, p] = acc[h, p] + buf[1, slot, h, p].astype(jnp.float32)

        out_ref[
            pl.ds(pl.multiple_of(h * BLOCK, BLOCK), BLOCK), pl.ds(pl.multiple_of(p * cp, cp), cp)
        ] = acc[h, p].astype(out_ref.dtype)
        return 0

    lax.fori_loop(0, nb_t * np_, last, 0)

    for b in range(nb_a):
        par_copy(b).wait_send()
    for i, m in remote:
        x_copy(i, m).wait_send()
        pass_on((x + i) % chips, m).wait_send()
    for i in range(1, A):
        dn_copy(i).wait_send()
        up_copy(i).wait_send()
    for b in range(nb_a):
        d, _ = s_dest(b)
        for i in range(1, A):
            s_copy(i, b).wait_send()

        @pl.when(d != t)
        def _():
            s_copy(0, b).wait_send()

    def drain(n, _):
        k, p = n // np_, n % np_
        for way in range(2):
            d, h = place(way, k)
            slot = d if way else d - 1

            @pl.when((d < t) if way else (d > t))
            def _():
                toward(way, slot, h, p).wait_send()

        return 0

    lax.fori_loop(0, steps * np_, drain, 0)


def on_device(tokens, query_weight, down, up, ids, live, slots):
    A, T = lax.axis_size("adapter"), lax.axis_size("tensor")
    rows_a, feat = tokens.shape
    cols = query_weight.shape[1]
    rank = down.shape[1]
    rows_d = rows_a * A // T
    cp = min(512, cols)
    np_ = cols // cp
    nb_a, nb_t = rows_a // BLOCK, rows_d // BLOCK
    chips = A // 2
    bf, f32 = jnp.bfloat16, jnp.float32
    dma = pltpu.SemaphoreType.DMA
    smem = pl.BlockSpec(memory_space=pltpu.SMEM)
    hbm = pl.BlockSpec(memory_space=pl.ANY)
    return pl.pallas_call(
        functools.partial(kernel, A, T),
        out_shape=jax.ShapeDtypeStruct((rows_d, cols), bf),
        in_specs=[smem, smem, smem, hbm, hbm, hbm, hbm],
        out_specs=pl.BlockSpec(memory_space=pltpu.VMEM),
        scratch_shapes=[
            pltpu.VMEM((A * nb_a, BLOCK, feat), bf),
            pltpu.VMEM((np_, feat, cp), bf),
            pltpu.VMEM(down.shape, bf),
            pltpu.VMEM(up.shape, bf),
            pltpu.VMEM((2, T - 1, nb_t, np_, BLOCK, cp), bf),
            pltpu.VMEM((nb_t, np_, BLOCK, cp), f32),
            pltpu.VMEM((A, nb_a, rank, feat), bf),
            pltpu.VMEM((A, nb_a, rank, feat), bf),
            pltpu.VMEM((A, nb_t, rank, cols), bf),
            pltpu.VMEM((A, nb_t, rank, cols), bf),
            pltpu.VMEM((nb_a, rank, BLOCK), bf),
            pltpu.VMEM((T, nb_t, rank, BLOCK), bf),
            dma((nb_a,)), dma((2,)), dma((np_,)),
            dma((nb_a,)), dma((nb_a,)),
            dma((chips, 2 * nb_a)), dma((chips, 2 * nb_a)),
            dma((chips, 2 * nb_a)), dma((chips, 2 * nb_a)),
            dma((A,)), dma((A,)), dma((A,)), dma((A,)),
            dma((A, nb_a)), dma((T, nb_t)),
            dma((2, T - 1, nb_t, np_)), dma((2, T - 1, nb_t, np_)),
            pltpu.SemaphoreType.REGULAR((2,)),
        ],
        compiler_params=pltpu.CompilerParams(
            collective_id=0, has_side_effects=True, vmem_limit_bytes=60 * 1024 * 1024
        ),
    )(ids, live, slots, tokens, query_weight, down, up)


def solution(mesh):
    placed = (
        P(("groups", "adapter"), "tensor"),
        P("tensor", "adapter"),
        P("adapter", None, "tensor"),
        P("adapter", None, None),
        P("groups"),
        P("groups"),
        P("groups"),
    )
    return jax.shard_map(
        on_device,
        mesh=mesh,
        in_specs=placed,
        out_specs=P(("groups", "tensor"), "adapter"),
        check_vma=False,
    )
```

```python
import functools

import jax
import jax.numpy as jnp
from jax import lax
from jax.experimental import pallas as pl
from jax.experimental.pallas import tpu as pltpu
from jax.sharding import PartitionSpec as P

BLOCK = 128
SCALE = 2.0
MESH = pl.DeviceIdType.MESH
PRE = 2
LAG = 3


def kernel(
    A, T,
    ids, live, slots, tok_hbm, w_hbm, dn_hbm, up_hbm, out_ref,
    tok, w, dn, up, buf, acc, dn_send, dn_recv, up_send, up_recv, s_send, s_recv,
    tok_sem, ld_sem, w_sem, par_ss, par_rs, x_ss, x_rs, f_ss, f_rs,
    dn_ss, dn_rs, up_ss, up_rs, s_ss, s_rs, fl_ss, fl_rs, ready,
):
    a = lax.axis_index("adapter")
    t = lax.axis_index("tensor")
    chips = A // 2
    x, core = a // 2, a % 2
    partner = 2 * x + 1 - core
    nb = tok.shape[0]
    nb_a, nb_t = nb // A, nb // T
    half = BLOCK // 2
    per_dev = dn_hbm.shape[0]
    np_, _, cp = w.shape
    cols = np_ * cp
    steps = (T - 1) * nb_t
    near = chips == 2 and nb_a == nb_t
    pre_n = min(PRE, np_) if near else 0

    def tok_load(b):
        return pltpu.make_async_copy(
            tok_hbm.at[pl.ds(b * BLOCK, BLOCK)], tok.at[a * nb_a + b], tok_sem.at[b]
        )

    def w_load(p):
        c = pl.ds(pl.multiple_of(p * cp, cp), cp)
        return pltpu.make_async_copy(w_hbm.at[:, c], w.at[p], w_sem.at[p])

    dn_load = pltpu.make_async_copy(dn_hbm, dn, ld_sem.at[0])
    up_load = pltpu.make_async_copy(up_hbm, up, ld_sem.at[1])

    tok_load(0).start()
    w_load(0).start()
    for b in range(1, nb_a):
        tok_load(b).start()
    for p in range(1, np_):
        w_load(p).start()
    dn_load.start()
    up_load.start()

    barrier = pltpu.get_barrier_semaphore()

    def greet(**to):
        pl.semaphore_signal(barrier, inc=1, device_id=to, device_id_type=MESH)

    @pl.when(t > 0)
    def _():
        greet(tensor=t - 1)

    @pl.when(t < T - 1)
    def _():
        greet(tensor=t + 1)

    for i in range(1, A):
        greet(adapter=(a + i) % A)

    if near:
        lead_r = jnp.where(a >= 1, a, 1)
        lead_l = jnp.where(a <= T - 2, a, T - 2)
        first_r = (T - 1 - lead_r) * nb_t
        first_l = lead_l * nb_t
        pre = jnp.logical_or(
            jnp.logical_and(t == 0, a >= 1), jnp.logical_and(t == T - 1, a <= T - 2)
        )
    else:
        first_r = first_l = 0

    def place(way, k):
        first = first_l if way else first_r
        m = jnp.where(k - 1 < first, k - 1, k)
        m = jnp.where(k == 0, first, m)
        d = m // nb_t
        return (d if way else T - 1 - d), m % nb_t

    def flow(way, to, slot, h, p):
        return pltpu.make_async_remote_copy(
            buf.at[way, slot, h, p], buf.at[way, slot, h, p],
            fl_ss.at[way, slot, h, p], fl_rs.at[way, slot, h, p],
            device_id={"tensor": to}, device_id_type=MESH,
        )

    right, left = (t + 1) % T, (t + T - 1) % T

    def toward(way, slot, h, p):
        return flow(way, left if way else right, slot, h, p)

    def base(q, p):
        return jnp.dot(tok[q], w[p], preferred_element_type=jnp.float32)

    if near:
        pre_way = jnp.where(t == 0, 0, 1)
        pre_slot = jnp.where(t == 0, jnp.maximum(a - 1, 0), jnp.minimum(a, T - 2))
        pre_to = jnp.where(t == 0, 1, T - 2)

    tok_load(0).wait()
    if pre_n:

        @pl.when(pre)
        def _():
            def one(p, _):
                w_load(p).wait()
                buf[pre_way, pre_slot, 0, p] = base(a * nb_a, p).astype(buf.dtype)
                return 0

            lax.fori_loop(0, pre_n, one, 0)

    for b in range(1, nb_a):
        tok_load(b).wait()

    ends = jnp.where(t > 0, 1, 0) + jnp.where(t < T - 1, 1, 0)
    pl.semaphore_wait(barrier, A - 1 + ends)

    if pre_n:

        @pl.when(pre)
        def _():
            for p in range(pre_n):
                flow(pre_way, pre_to, pre_slot, 0, p).start()

    def par_copy(b):
        r = tok.at[a * nb_a + b]
        return pltpu.make_async_remote_copy(
            r, r, par_ss.at[b], par_rs.at[b], device_id={"adapter": partner}, device_id_type=MESH
        )

    def lead_core(c):
        return jnp.where(2 * c >= chips, 1, 0)

    def row_block(c, m):
        k = jnp.where(m < nb_a, lead_core(c), 1 - lead_core(c))
        return (2 * c + k) * nb_a + m % nb_a, k

    def part(q, k):
        return tok.at[q, pl.ds(pl.multiple_of(k * half, half), half)]

    def x_copy(i, m):
        r = part(row_block(x, m)[0], core)
        return pltpu.make_async_remote_copy(
            r, r, x_ss.at[i, m], x_rs.at[x, m],
            device_id={"adapter": 2 * ((x + i) % chips) + core}, device_id_type=MESH,
        )

    def x_arrival(c, m):
        r = part(row_block(c, m)[0], core)
        return pltpu.make_async_remote_copy(
            r, r, x_ss.at[0, m], x_rs.at[c, m],
            device_id={"adapter": partner}, device_id_type=MESH,
        )

    def pass_on(c, m):
        r = part(row_block(c, m)[0], core)
        return pltpu.make_async_remote_copy(
            r, r, f_ss.at[c, m], f_rs.at[c, m],
            device_id={"adapter": partner}, device_id_type=MESH,
        )

    for b in range(nb_a):
        par_copy(b).start()
    for m in range(2 * nb_a):

        @pl.when(row_block(x, m)[1] != core)
        def _():
            par_copy(m % nb_a).wait_recv()

        for i in range(1, chips):
            x_copy(i, m).start()

    def fetch(c, m):
        x_arrival(c, m).wait_recv()
        pass_on(c, m).start()

    def fetched(c, m):
        pass_on(c, m).wait_recv()

    def tell(i, to):
        pl.semaphore_signal(ready.at[i], inc=1, device_id={"tensor": to}, device_id_type=MESH)

    @pl.when(t == 0)
    def _():
        tell(0, right)

    @pl.when(t == T - 1)
    def _():
        tell(1, left)

    def relay():
        @pl.when(jnp.logical_and(t > 0, t < T - 1))
        def _():
            pl.semaphore_wait(ready.at[0], 1)
            tell(0, right)
            pl.semaphore_wait(ready.at[1], 1)
            tell(1, left)

    def all_in():
        @pl.when(t == 0)
        def _():
            pl.semaphore_wait(ready.at[1], 1)

        @pl.when(t == T - 1)
        def _():
            pl.semaphore_wait(ready.at[0], 1)

    def slot_of(k):
        return slots[ids[k]]

    def dn_copy(i):
        to = (a + i) % A
        return pltpu.make_async_remote_copy(
            dn_send.at[to], dn_recv.at[a], dn_ss.at[i], dn_rs.at[i],
            device_id={"adapter": to}, device_id_type=MESH,
        )

    def up_copy(i):
        to = (a + i) % A
        return pltpu.make_async_remote_copy(
            up_send.at[to], up_recv.at[a], up_ss.at[i], up_rs.at[i],
            device_id={"adapter": to}, device_id_type=MESH,
        )

    def s_dest(b):
        k = a * nb_a + b
        return k // nb_t, k % nb_t

    def s_copy(i, b):
        d, kk = s_dest(b)
        return pltpu.make_async_remote_copy(
            s_send.at[b], s_recv.at[t, kk], s_ss.at[i, b], s_rs.at[t, kk],
            device_id={"adapter": (a + i) % A, "tensor": d}, device_id_type=MESH,
        )

    def send_adapters():
        dn_load.wait()
        for i in range(A):
            for b in range(nb_a):
                dn_send[i, b] = dn[lax.rem(slot_of(i * nb_a + b), per_dev)]
        dn_recv[a] = dn_send[a]
        for i in range(1, A):
            dn_copy(i).start()
        up_load.wait()
        for b in range(nb_t):
            sl = lax.rem(slot_of(t * nb_t + b), per_dev)
            for i in range(A):
                up_send[i, b] = up[sl, :, i * cols:(i + 1) * cols]
        up_recv[a] = up_send[a]
        for i in range(1, A):
            up_copy(i).start()

    def send_shrunk():
        all_in()
        for i in range(1, A):
            dn_copy(i).wait_recv()
        for b in range(nb_a):
            k = a * nb_a + b
            mine = dn_recv[lax.div(slot_of(k), per_dev), b]
            s = lax.dot_general(
                mine, tok[k], (((1,), (1,)), ((), ())), preferred_element_type=jnp.float32
            )
            keep = lax.broadcasted_iota(jnp.int32, s.shape, 1) < live[k]
            s_send[b] = jnp.where(keep, s, 0.0).astype(s_send.dtype)
            d, kk = s_dest(b)
            for i in range(A):
                if i:
                    s_copy(i, b).start()
                else:
                    @pl.when(d == t)
                    def _():
                        s_recv[t, kk] = s_send[b]

                    @pl.when(d != t)
                    def _():
                        s_copy(0, b).start()

    def wait_adapters():
        for i in range(1, A):
            up_copy(i).wait_recv()
        for b in range(nb_t):
            owner = (t * nb_t + b) // nb_a
            for tt in range(T):
                c = pltpu.make_async_remote_copy(
                    s_send.at[0], s_recv.at[tt, b], s_ss.at[0, 0], s_rs.at[tt, b],
                    device_id={"adapter": partner}, device_id_type=MESH,
                )

                @pl.when(jnp.logical_or(owner != a, t != tt))
                def _():
                    c.wait_recv()

    remote = [(i, m) for i in range(1, chips) for m in range(2 * nb_a)]
    if not near:
        for i, m in remote:
            fetch((x + i) % chips, m)
        for i, m in remote:
            fetched((x + i) % chips, m)

    units = steps * np_
    lags = (LAG * t, LAG * (T - 1 - t))

    def advance(way, n):
        m = n - lags[way]
        inside = jnp.logical_and(m >= 0, m < units)
        m = jnp.clip(m, 0, units - 1)
        k, p = m // np_, m % np_
        d, h = place(way, k)
        slot = d if way else d - 1
        go = jnp.logical_and(inside, (d < t) if way else (d > t))
        if pre_n:
            go = jnp.logical_and(go, jnp.logical_not(jnp.logical_and(pre, m < pre_n)))

        @pl.when(go)
        def _():
            mine = base(d * nb_t + h, p)
            fresh = (t == T - 1) if way else (t == 0)

            @pl.when(fresh)
            def _():
                buf[way, slot, h, p] = mine.astype(buf.dtype)

            @pl.when(jnp.logical_not(fresh))
            def _():
                toward(way, slot, h, p).wait_recv()
                buf[way, slot, h, p] = (
                    mine + buf[way, slot, h, p].astype(jnp.float32)
                ).astype(buf.dtype)

            toward(way, slot, h, p).start()

    def iteration(n, _):
        k, p = n // np_, n % np_
        if near:

            @pl.when(jnp.logical_and(p == 0, jnp.logical_and(k >= 1, k <= 2 * nb_a)))
            def _():
                fetch(1 - x, k - 1)
                fetched(1 - x, k - 1)

        @pl.when(n == min(1, steps - 1) * np_)
        def _():
            relay()

        @pl.when(n == min(2, steps - 1) * np_)
        def _():
            send_adapters()

        @pl.when(n == max(steps - 2, 0) * np_)
        def _():
            send_shrunk()

        loaded = k == 0
        if pre_n:
            loaded = jnp.logical_and(
                loaded, jnp.logical_not(jnp.logical_and(pre, p < pre_n))
            )

        @pl.when(loaded)
        def _():
            w_load(p).wait()

        advance(0, n)
        advance(1, n)
        h = k - (steps - nb_t)

        @pl.when(jnp.logical_and(h >= 0, h < nb_t))
        def _():
            acc[h, p] = base(t * nb_t + h, p)

        return 0

    lax.fori_loop(0, units + LAG * (T - 2), iteration, 0)
    wait_adapters()

    def last(n, _):
        h, p = n // np_, n % np_
        own = lax.div(slot_of(t * nb_t + h), per_dev)
        u = up_recv[own, h, :, pl.ds(pl.multiple_of(p * cp, cp), cp)]
        lhs = s_recv[:, h].reshape(T * s_recv.shape[2], BLOCK)
        acc[h, p] = acc[h, p] + SCALE * lax.dot_general(
            lhs, jnp.concatenate([u] * T, axis=0), (((0,), (0,)), ((), ())),
            preferred_element_type=jnp.float32,
        )

        @pl.when(t > 0)
        def _():
            slot = jnp.maximum(t - 1, 0)
            toward(0, slot, h, p).wait_recv()
            acc[h, p] = acc[h, p] + buf[0, slot, h, p].astype(jnp.float32)

        @pl.when(t < T - 1)
        def _():
            slot = jnp.minimum(t, T - 2)
            toward(1, slot, h, p).wait_recv()
            acc[h, p] = acc[h, p] + buf[1, slot, h, p].astype(jnp.float32)

        out_ref[
            pl.ds(pl.multiple_of(h * BLOCK, BLOCK), BLOCK), pl.ds(pl.multiple_of(p * cp, cp), cp)
        ] = acc[h, p].astype(out_ref.dtype)
        return 0

    lax.fori_loop(0, nb_t * np_, last, 0)

    for b in range(nb_a):
        par_copy(b).wait_send()
    for i, m in remote:
        x_copy(i, m).wait_send()
        pass_on((x + i) % chips, m).wait_send()
    for i in range(1, A):
        dn_copy(i).wait_send()
        up_copy(i).wait_send()
    for b in range(nb_a):
        d, _ = s_dest(b)
        for i in range(1, A):
            s_copy(i, b).wait_send()

        @pl.when(d != t)
        def _():
            s_copy(0, b).wait_send()

    def drain(n, _):
        k, p = n // np_, n % np_
        for way in range(2):
            d, h = place(way, k)
            slot = d if way else d - 1

            @pl.when((d < t) if way else (d > t))
            def _():
                toward(way, slot, h, p).wait_send()

        return 0

    lax.fori_loop(0, steps * np_, drain, 0)


def on_device(tokens, query_weight, down, up, ids, live, slots):
    A, T = lax.axis_size("adapter"), lax.axis_size("tensor")
    rows_a, feat = tokens.shape
    cols = query_weight.shape[1]
    rank = down.shape[1]
    rows_d = rows_a * A // T
    cp = min(512, cols)
    np_ = cols // cp
    nb_a, nb_t = rows_a // BLOCK, rows_d // BLOCK
    chips = A // 2
    bf, f32 = jnp.bfloat16, jnp.float32
    dma = pltpu.SemaphoreType.DMA
    smem = pl.BlockSpec(memory_space=pltpu.SMEM)
    hbm = pl.BlockSpec(memory_space=pl.ANY)
    return pl.pallas_call(
        functools.partial(kernel, A, T),
        out_shape=jax.ShapeDtypeStruct((rows_d, cols), bf),
        in_specs=[smem, smem, smem, hbm, hbm, hbm, hbm],
        out_specs=pl.BlockSpec(memory_space=pltpu.VMEM),
        scratch_shapes=[
            pltpu.VMEM((A * nb_a, BLOCK, feat), bf),
            pltpu.VMEM((np_, feat, cp), bf),
            pltpu.VMEM(down.shape, bf),
            pltpu.VMEM(up.shape, bf),
            pltpu.VMEM((2, T - 1, nb_t, np_, BLOCK, cp), bf),
            pltpu.VMEM((nb_t, np_, BLOCK, cp), f32),
            pltpu.VMEM((A, nb_a, rank, feat), bf),
            pltpu.VMEM((A, nb_a, rank, feat), bf),
            pltpu.VMEM((A, nb_t, rank, cols), bf),
            pltpu.VMEM((A, nb_t, rank, cols), bf),
            pltpu.VMEM((nb_a, rank, BLOCK), bf),
            pltpu.VMEM((T, nb_t, rank, BLOCK), bf),
            dma((nb_a,)), dma((2,)), dma((np_,)),
            dma((nb_a,)), dma((nb_a,)),
            dma((chips, 2 * nb_a)), dma((chips, 2 * nb_a)),
            dma((chips, 2 * nb_a)), dma((chips, 2 * nb_a)),
            dma((A,)), dma((A,)), dma((A,)), dma((A,)),
            dma((A, nb_a)), dma((T, nb_t)),
            dma((2, T - 1, nb_t, np_)), dma((2, T - 1, nb_t, np_)),
            pltpu.SemaphoreType.REGULAR((2,)),
        ],
        compiler_params=pltpu.CompilerParams(
            collective_id=0, has_side_effects=True, vmem_limit_bytes=60 * 1024 * 1024
        ),
    )(ids, live, slots, tokens, query_weight, down, up)


def solution(mesh):
    placed = (
        P(("groups", "adapter"), "tensor"),
        P("tensor", "adapter"),
        P("adapter", None, "tensor"),
        P("adapter", None, None),
        P("groups"),
        P("groups"),
        P("groups"),
    )
    return jax.shard_map(
        on_device,
        mesh=mesh,
        in_specs=placed,
        out_specs=P(("groups", "tensor"), "adapter"),
        check_vma=False,
    )
```

```python
import functools

import jax
import jax.numpy as jnp
from jax import lax
from jax.experimental import pallas as pl
from jax.experimental.pallas import tpu as pltpu
from jax.sharding import PartitionSpec as P

BLOCK = 128
SCALE = 2.0
MESH = pl.DeviceIdType.MESH
PRE = (2, 1)
LAG = 3


def kernel(
    A, T,
    ids, live, slots, tok_hbm, w_hbm, dn_hbm, up_hbm, out_ref,
    tok, w, dn, up, buf, acc, dn_send, dn_recv, up_send, up_recv, s_send, s_recv,
    tok_sem, ld_sem, w_sem, par_ss, par_rs, x_ss, x_rs, f_ss, f_rs,
    dn_ss, dn_rs, up_ss, up_rs, s_ss, s_rs, fl_ss, fl_rs, ready,
):
    a = lax.axis_index("adapter")
    t = lax.axis_index("tensor")
    chips = A // 2
    x, core = a // 2, a % 2
    partner = 2 * x + 1 - core
    nb = tok.shape[0]
    nb_a, nb_t = nb // A, nb // T
    half = BLOCK // 2
    per_dev = dn_hbm.shape[0]
    np_, _, cp = w.shape
    cols = np_ * cp
    steps = (T - 1) * nb_t
    near = chips == 2 and nb_a == nb_t

    def tok_load(b):
        return pltpu.make_async_copy(
            tok_hbm.at[pl.ds(b * BLOCK, BLOCK)], tok.at[a * nb_a + b], tok_sem.at[b]
        )

    def w_load(p):
        c = pl.ds(pl.multiple_of(p * cp, cp), cp)
        return pltpu.make_async_copy(w_hbm.at[:, c], w.at[p], w_sem.at[p])

    dn_load = pltpu.make_async_copy(dn_hbm, dn, ld_sem.at[0])
    up_load = pltpu.make_async_copy(up_hbm, up, ld_sem.at[1])

    tok_load(0).start()
    w_load(0).start()
    for b in range(1, nb_a):
        tok_load(b).start()
    for p in range(1, np_):
        w_load(p).start()
    dn_load.start()
    up_load.start()

    barrier = pltpu.get_barrier_semaphore()

    def greet(**to):
        pl.semaphore_signal(barrier, inc=1, device_id=to, device_id_type=MESH)

    @pl.when(t > 0)
    def _():
        greet(tensor=t - 1)

    @pl.when(t < T - 1)
    def _():
        greet(tensor=t + 1)

    for i in range(1, A):
        greet(adapter=(a + i) % A)

    if near:
        lead_r = jnp.where(a >= 1, a, 1)
        lead_l = jnp.where(a <= T - 2, a, T - 2)
        first_r = (T - 1 - lead_r) * nb_t
        first_l = lead_l * nb_t
        pre = jnp.logical_or(
            jnp.logical_and(t == 0, a >= 1), jnp.logical_and(t == T - 1, a <= T - 2)
        )
    else:
        first_r = first_l = 0

    def place(way, k):
        first = first_l if way else first_r
        m = jnp.where(k - 1 < first, k - 1, k)
        m = jnp.where(k == 0, first, m)
        d = m // nb_t
        return (d if way else T - 1 - d), m % nb_t

    def flow(way, to, slot, h, p):
        return pltpu.make_async_remote_copy(
            buf.at[way, slot, h, p], buf.at[way, slot, h, p],
            fl_ss.at[way, slot], fl_rs.at[way, slot, h, p],
            device_id={"tensor": to}, device_id_type=MESH,
        )

    right, left = (t + 1) % T, (t + T - 1) % T

    def toward(way, slot, h, p):
        return flow(way, left if way else right, slot, h, p)

    def base(q, p):
        return jnp.dot(tok[q], w[p], preferred_element_type=jnp.float32)

    if near:
        pre_way = jnp.where(t == 0, 0, 1)
        pre_slot = jnp.where(t == 0, jnp.maximum(a - 1, 0), jnp.minimum(a, T - 2))
        pre_to = jnp.where(t == 0, 1, T - 2)

    def lead_unit(p):
        w_load(p).wait()
        buf[pre_way, pre_slot, 0, p] = base(a * nb_a, p).astype(buf.dtype)

    tok_load(0).wait()
    if near:
        early = jnp.where(t == 0, min(PRE[0], np_), min(PRE[1], np_))

        @pl.when(pre)
        def _():
            def one(p, _):
                lead_unit(p)
                return 0

            lax.fori_loop(0, early, one, 0)

    for b in range(1, nb_a):
        tok_load(b).wait()

    ends = jnp.where(t > 0, 1, 0) + jnp.where(t < T - 1, 1, 0)
    pl.semaphore_wait(barrier, A - 1 + ends)

    def par_copy(b):
        r = tok.at[a * nb_a + b]
        return pltpu.make_async_remote_copy(
            r, r, par_ss.at[b], par_rs.at[b], device_id={"adapter": partner}, device_id_type=MESH
        )

    def lead_core(c):
        return jnp.where(2 * c >= chips, 1, 0)

    def row_block(c, m):
        k = jnp.where(m < nb_a, lead_core(c), 1 - lead_core(c))
        return (2 * c + k) * nb_a + m % nb_a, k

    def part(q, k):
        return tok.at[q, pl.ds(pl.multiple_of(k * half, half), half)]

    def x_copy(i, m):
        r = part(row_block(x, m)[0], core)
        return pltpu.make_async_remote_copy(
            r, r, x_ss.at[i, m], x_rs.at[x, m],
            device_id={"adapter": 2 * ((x + i) % chips) + core}, device_id_type=MESH,
        )

    def x_arrival(c, m):
        r = part(row_block(c, m)[0], core)
        return pltpu.make_async_remote_copy(
            r, r, x_ss.at[0, m], x_rs.at[c, m],
            device_id={"adapter": partner}, device_id_type=MESH,
        )

    def pass_on(c, m):
        r = part(row_block(c, m)[0], core)
        return pltpu.make_async_remote_copy(
            r, r, f_ss.at[c, m], f_rs.at[c, m],
            device_id={"adapter": partner}, device_id_type=MESH,
        )

    def send_x(m):
        for i in range(1, chips):
            x_copy(i, m).start()

    if near:

        @pl.when(pre)
        def _():
            def one(p, _):
                flow(pre_way, pre_to, pre_slot, 0, p).start()
                return 0

            lax.fori_loop(0, early, one, 0)

    for b in range(nb_a):
        par_copy(b).start()

    own_first = lead_core(x) == core

    @pl.when(own_first)
    def _():
        for m in range(nb_a):
            send_x(m)

    if near:

        @pl.when(pre)
        def _():
            def one(p, _):
                lead_unit(p)
                flow(pre_way, pre_to, pre_slot, 0, p).start()
                return 0

            lax.fori_loop(early, np_, one, 0)

    for b in range(nb_a):
        par_copy(b).wait_recv()

        @pl.when(own_first)
        def _():
            send_x(nb_a + b)

        @pl.when(jnp.logical_not(own_first))
        def _():
            send_x(b)

    @pl.when(jnp.logical_not(own_first))
    def _():
        for m in range(nb_a, 2 * nb_a):
            send_x(m)

    def fetch(c, m):
        x_arrival(c, m).wait_recv()
        pass_on(c, m).start()

    def fetched(c, m):
        pass_on(c, m).wait_recv()

    def tell(i, to):
        pl.semaphore_signal(ready.at[i], inc=1, device_id={"tensor": to}, device_id_type=MESH)

    @pl.when(t == 0)
    def _():
        tell(0, right)

    @pl.when(t == T - 1)
    def _():
        tell(1, left)

    def relay():
        @pl.when(jnp.logical_and(t > 0, t < T - 1))
        def _():
            pl.semaphore_wait(ready.at[0], 1)
            tell(0, right)
            pl.semaphore_wait(ready.at[1], 1)
            tell(1, left)

    def all_in():
        @pl.when(t == 0)
        def _():
            pl.semaphore_wait(ready.at[1], 1)

        @pl.when(t == T - 1)
        def _():
            pl.semaphore_wait(ready.at[0], 1)

    def slot_of(k):
        return slots[ids[k]]

    def dn_copy(i):
        to = (a + i) % A
        return pltpu.make_async_remote_copy(
            dn_send.at[to], dn_recv.at[a], dn_ss.at[i], dn_rs.at[i],
            device_id={"adapter": to}, device_id_type=MESH,
        )

    def up_copy(i):
        to = (a + i) % A
        return pltpu.make_async_remote_copy(
            up_send.at[to], up_recv.at[a], up_ss.at[i], up_rs.at[i],
            device_id={"adapter": to}, device_id_type=MESH,
        )

    def s_dest(b):
        k = a * nb_a + b
        return k // nb_t, k % nb_t

    def s_copy(i, b):
        d, kk = s_dest(b)
        return pltpu.make_async_remote_copy(
            s_send.at[b], s_recv.at[t, kk], s_ss.at[i, b], s_rs.at[t, kk],
            device_id={"adapter": (a + i) % A, "tensor": d}, device_id_type=MESH,
        )

    def send_adapters():
        dn_load.wait()
        for i in range(A):
            for b in range(nb_a):
                dn_send[i, b] = dn[lax.rem(slot_of(i * nb_a + b), per_dev)]
        dn_recv[a] = dn_send[a]
        for i in range(1, A):
            dn_copy(i).start()
        up_load.wait()
        for b in range(nb_t):
            sl = lax.rem(slot_of(t * nb_t + b), per_dev)
            for i in range(A):
                up_send[i, b] = up[sl, :, i * cols:(i + 1) * cols]
        up_recv[a] = up_send[a]
        for i in range(1, A):
            up_copy(i).start()

    def send_shrunk():
        all_in()
        for i in range(1, A):
            dn_copy(i).wait_recv()
        for b in range(nb_a):
            k = a * nb_a + b
            mine = dn_recv[lax.div(slot_of(k), per_dev), b]
            s = lax.dot_general(
                mine, tok[k], (((1,), (1,)), ((), ())), preferred_element_type=jnp.float32
            )
            keep = lax.broadcasted_iota(jnp.int32, s.shape, 1) < live[k]
            s_send[b] = jnp.where(keep, s, 0.0).astype(s_send.dtype)
            d, kk = s_dest(b)
            for i in range(A):
                if i:
                    s_copy(i, b).start()
                else:
                    @pl.when(d == t)
                    def _():
                        s_recv[t, kk] = s_send[b]

                    @pl.when(d != t)
                    def _():
                        s_copy(0, b).start()

    def wait_adapters():
        for i in range(1, A):
            up_copy(i).wait_recv()
        for b in range(nb_t):
            owner = (t * nb_t + b) // nb_a
            for tt in range(T):
                c = pltpu.make_async_remote_copy(
                    s_send.at[0], s_recv.at[tt, b], s_ss.at[0, 0], s_rs.at[tt, b],
                    device_id={"adapter": partner}, device_id_type=MESH,
                )

                @pl.when(jnp.logical_or(owner != a, t != tt))
                def _():
                    c.wait_recv()

    remote = [(i, m) for i in range(1, chips) for m in range(2 * nb_a)]
    if not near:
        for i, m in remote:
            fetch((x + i) % chips, m)
        for i, m in remote:
            fetched((x + i) % chips, m)

    units = steps * np_
    lags = (LAG * t, LAG * (T - 1 - t))

    def advance(way, n):
        m = n - lags[way]
        inside = jnp.logical_and(m >= 0, m < units)
        m = jnp.clip(m, 0, units - 1)
        k, p = m // np_, m % np_
        d, h = place(way, k)
        slot = d if way else d - 1
        go = jnp.logical_and(inside, (d < t) if way else (d > t))
        if near:
            go = jnp.logical_and(go, jnp.logical_not(jnp.logical_and(pre, m < np_)))

        @pl.when(go)
        def _():
            mine = base(d * nb_t + h, p)
            fresh = (t == T - 1) if way else (t == 0)

            @pl.when(fresh)
            def _():
                buf[way, slot, h, p] = mine.astype(buf.dtype)

            @pl.when(jnp.logical_not(fresh))
            def _():
                toward(way, slot, h, p).wait_recv()
                buf[way, slot, h, p] = (
                    mine + buf[way, slot, h, p].astype(jnp.float32)
                ).astype(buf.dtype)

            toward(way, slot, h, p).start()

    def iteration(n, _):
        k, p = n // np_, n % np_
        if near:

            @pl.when(jnp.logical_and(p == 0, jnp.logical_and(k >= 1, k <= 2 * nb_a)))
            def _():
                fetch(1 - x, k - 1)
                fetched(1 - x, k - 1)

        @pl.when(n == min(1, steps - 1) * np_)
        def _():
            relay()

        @pl.when(n == min(2, steps - 1) * np_)
        def _():
            send_adapters()

        @pl.when(n == max(steps - 2, 0) * np_)
        def _():
            send_shrunk()

        loaded = k == 0
        if near:
            loaded = jnp.logical_and(loaded, jnp.logical_not(pre))

        @pl.when(loaded)
        def _():
            w_load(p).wait()

        advance(0, n)
        advance(1, n)
        h = k - (steps - nb_t)

        @pl.when(jnp.logical_and(h >= 0, h < nb_t))
        def _():
            acc[h, p] = base(t * nb_t + h, p)

        return 0

    lax.fori_loop(0, units + LAG * (T - 2), iteration, 0)
    wait_adapters()
    for b in range(nb_a):
        par_copy(b).wait_send()
    for i, m in remote:
        x_copy(i, m).wait_send()
        pass_on((x + i) % chips, m).wait_send()
    for i in range(1, A):
        dn_copy(i).wait_send()
        up_copy(i).wait_send()
    for b in range(nb_a):
        d, _ = s_dest(b)
        for i in range(1, A):
            s_copy(i, b).wait_send()

        @pl.when(d != t)
        def _():
            s_copy(0, b).wait_send()

    def last(n, _):
        h, p = n // np_, n % np_
        own = lax.div(slot_of(t * nb_t + h), per_dev)
        u = up_recv[own, h, :, pl.ds(pl.multiple_of(p * cp, cp), cp)]
        lhs = s_recv[:, h].reshape(T * s_recv.shape[2], BLOCK)
        acc[h, p] = acc[h, p] + SCALE * lax.dot_general(
            lhs, jnp.concatenate([u] * T, axis=0), (((0,), (0,)), ((), ())),
            preferred_element_type=jnp.float32,
        )

        @pl.when(t > 0)
        def _():
            slot = jnp.maximum(t - 1, 0)
            toward(0, slot, h, p).wait_recv()
            acc[h, p] = acc[h, p] + buf[0, slot, h, p].astype(jnp.float32)

        @pl.when(t < T - 1)
        def _():
            slot = jnp.minimum(t, T - 2)
            toward(1, slot, h, p).wait_recv()
            acc[h, p] = acc[h, p] + buf[1, slot, h, p].astype(jnp.float32)

        out_ref[
            pl.ds(pl.multiple_of(h * BLOCK, BLOCK), BLOCK), pl.ds(pl.multiple_of(p * cp, cp), cp)
        ] = acc[h, p].astype(out_ref.dtype)
        return 0

    lax.fori_loop(0, nb_t * np_, last, 0)

    for way in range(2):
        for slot in range(T - 1):

            @pl.when((slot < t) if way else (slot + 1 > t))
            def _():
                pltpu.make_async_remote_copy(
                    buf.at[way, slot], buf.at[way, slot],
                    fl_ss.at[way, slot], fl_rs.at[way, slot, 0, 0],
                    device_id={"tensor": left if way else right}, device_id_type=MESH,
                ).wait_send()


def on_device(tokens, query_weight, down, up, ids, live, slots):
    A, T = lax.axis_size("adapter"), lax.axis_size("tensor")
    rows_a, feat = tokens.shape
    cols = query_weight.shape[1]
    rank = down.shape[1]
    rows_d = rows_a * A // T
    cp = min(512, cols)
    np_ = cols // cp
    nb_a, nb_t = rows_a // BLOCK, rows_d // BLOCK
    chips = A // 2
    bf, f32 = jnp.bfloat16, jnp.float32
    dma = pltpu.SemaphoreType.DMA
    smem = pl.BlockSpec(memory_space=pltpu.SMEM)
    hbm = pl.BlockSpec(memory_space=pl.ANY)
    return pl.pallas_call(
        functools.partial(kernel, A, T),
        out_shape=pltpu.VMEM((rows_d, cols), bf),
        in_specs=[smem, smem, smem, hbm, hbm, hbm, hbm],
        out_specs=pl.BlockSpec(memory_space=pltpu.VMEM),
        scratch_shapes=[
            pltpu.VMEM((A * nb_a, BLOCK, feat), bf),
            pltpu.VMEM((np_, feat, cp), bf),
            pltpu.VMEM(down.shape, bf),
            pltpu.VMEM(up.shape, bf),
            pltpu.VMEM((2, T - 1, nb_t, np_, BLOCK, cp), bf),
            pltpu.VMEM((nb_t, np_, BLOCK, cp), f32),
            pltpu.VMEM((A, nb_a, rank, feat), bf),
            pltpu.VMEM((A, nb_a, rank, feat), bf),
            pltpu.VMEM((A, nb_t, rank, cols), bf),
            pltpu.VMEM((A, nb_t, rank, cols), bf),
            pltpu.VMEM((nb_a, rank, BLOCK), bf),
            pltpu.VMEM((T, nb_t, rank, BLOCK), bf),
            dma((nb_a,)), dma((2,)), dma((np_,)),
            dma((nb_a,)), dma((nb_a,)),
            dma((chips, 2 * nb_a)), dma((chips, 2 * nb_a)),
            dma((chips, 2 * nb_a)), dma((chips, 2 * nb_a)),
            dma((A,)), dma((A,)), dma((A,)), dma((A,)),
            dma((A, nb_a)), dma((T, nb_t)),
            dma((2, T - 1)), dma((2, T - 1, nb_t, np_)),
            pltpu.SemaphoreType.REGULAR((2,)),
        ],
        compiler_params=pltpu.CompilerParams(
            collective_id=0, has_side_effects=True, vmem_limit_bytes=60 * 1024 * 1024
        ),
    )(ids, live, slots, tokens, query_weight, down, up)


def solution(mesh):
    placed = (
        P(("groups", "adapter"), "tensor"),
        P("tensor", "adapter"),
        P("adapter", None, "tensor"),
        P("adapter", None, None),
        P("groups"),
        P("groups"),
        P("groups"),
    )
    return jax.shard_map(
        on_device,
        mesh=mesh,
        in_specs=placed,
        out_specs=P(("groups", "tensor"), "adapter"),
        check_vma=False,
    )
```

```python
import functools

import jax
import jax.numpy as jnp
from jax import lax
from jax.experimental import pallas as pl
from jax.experimental.pallas import tpu as pltpu
from jax.sharding import PartitionSpec as P

BLOCK = 128
SCALE = 2.0
MESH = pl.DeviceIdType.MESH
PRE = 1
LAG = 3


def kernel(
    A, T,
    ids_hbm, live_hbm, slots_hbm, tok_hbm, w_hbm, dn_hbm, up_hbm, out_ref,
    ids, live, slots, tok, w, dn, up, buf, acc, dn_send, dn_recv, up_send, up_recv, s_send, s_recv,
    sm_sem, tok_sem, ld_sem, w_sem, par_ss, par_rs, x_ss, x_rs, f_ss, f_rs,
    dn_ss, dn_rs, up_ss, up_rs, s_ss, s_rs, fl_ss, fl_rs, ready,
):
    a = lax.axis_index("adapter")
    t = lax.axis_index("tensor")
    chips = A // 2
    x, core = a // 2, a % 2
    partner = 2 * x + 1 - core
    nb = tok.shape[0]
    nb_a, nb_t = nb // A, nb // T
    half = BLOCK // 2
    per_dev = dn_hbm.shape[0]
    np_, _, cp = w.shape
    cols = np_ * cp
    steps = (T - 1) * nb_t
    near = chips == 2 and nb_a == nb_t

    def tok_load(b):
        return pltpu.make_async_copy(
            tok_hbm.at[pl.ds(b * BLOCK, BLOCK)], tok.at[a * nb_a + b], tok_sem.at[b]
        )

    def w_load(p):
        c = pl.ds(pl.multiple_of(p * cp, cp), cp)
        return pltpu.make_async_copy(w_hbm.at[:, c], w.at[p], w_sem.at[p])

    dn_load = pltpu.make_async_copy(dn_hbm, dn, ld_sem.at[0])
    up_load = pltpu.make_async_copy(up_hbm, up, ld_sem.at[1])

    tok_load(0).start()
    w_load(0).start()

    barrier = pltpu.get_barrier_semaphore()

    def greet(**to):
        pl.semaphore_signal(barrier, inc=1, device_id=to, device_id_type=MESH)

    @pl.when(t > 0)
    def _():
        greet(tensor=t - 1)

    @pl.when(t < T - 1)
    def _():
        greet(tensor=t + 1)

    for i in range(1, A):
        greet(adapter=(a + i) % A)

    if near:
        lead_r = jnp.where(a >= 1, a, 1)
        lead_l = jnp.where(a <= T - 2, a, T - 2)
        first_r = (T - 1 - lead_r) * nb_t
        first_l = lead_l * nb_t
        pre = jnp.logical_or(
            jnp.logical_and(t == 0, a >= 1), jnp.logical_and(t == T - 1, a <= T - 2)
        )
    else:
        first_r = first_l = 0

    def place(way, k):
        first = first_l if way else first_r
        m = jnp.where(k - 1 < first, k - 1, k)
        m = jnp.where(k == 0, first, m)
        d = m // nb_t
        return (d if way else T - 1 - d), m % nb_t

    def flow(way, to, slot, h, p):
        return pltpu.make_async_remote_copy(
            buf.at[way, slot, h, p], buf.at[way, slot, h, p],
            fl_ss.at[way, slot], fl_rs.at[way, slot, h, p],
            device_id={"tensor": to}, device_id_type=MESH,
        )

    right, left = (t + 1) % T, (t + T - 1) % T

    def toward(way, slot, h, p):
        return flow(way, left if way else right, slot, h, p)

    def base(q, p):
        return jnp.dot(tok[q], w[p], preferred_element_type=jnp.float32)

    early = min(PRE, np_)
    if near:
        pre_way = jnp.where(t == 0, 0, 1)
        pre_slot = jnp.where(t == 0, jnp.maximum(a - 1, 0), jnp.minimum(a, T - 2))
        pre_to = jnp.where(t == 0, 1, T - 2)

    def lead_unit(p):
        w_load(p).wait()
        buf[pre_way, pre_slot, 0, p] = base(a * nb_a, p).astype(buf.dtype)

    tok_load(0).wait()
    for b in range(1, nb_a):
        tok_load(b).start()
    for p in range(1, min(2, np_)):
        w_load(p).start()

    if near:
        @pl.when(pre)
        def _():
            for p in range(early):
                lead_unit(p)

    for p in range(2, np_):
        w_load(p).start()

    ends = jnp.where(t > 0, 1, 0) + jnp.where(t < T - 1, 1, 0)
    pl.semaphore_wait(barrier, A - 1 + ends)

    def par_copy(b, k):
        r = part(a * nb_a + b, k)
        return pltpu.make_async_remote_copy(
            r, r, par_ss.at[b, k], par_rs.at[b, k],
            device_id={"adapter": partner}, device_id_type=MESH,
        )

    def lead_core(c):
        return jnp.where(2 * c >= chips, 1, 0)

    def row_block(c, m):
        k = jnp.where(m < nb_a, lead_core(c), 1 - lead_core(c))
        return (2 * c + k) * nb_a + m % nb_a, k

    def part(q, k):
        return tok.at[q, pl.ds(pl.multiple_of(k * half, half), half)]

    def x_copy(i, m):
        r = part(row_block(x, m)[0], core)
        return pltpu.make_async_remote_copy(
            r, r, x_ss.at[i, m], x_rs.at[x, m],
            device_id={"adapter": 2 * ((x + i) % chips) + core}, device_id_type=MESH,
        )

    def x_arrival(c, m):
        r = part(row_block(c, m)[0], core)
        return pltpu.make_async_remote_copy(
            r, r, x_ss.at[0, m], x_rs.at[c, m],
            device_id={"adapter": partner}, device_id_type=MESH,
        )

    def pass_on(c, m):
        r = part(row_block(c, m)[0], core)
        return pltpu.make_async_remote_copy(
            r, r, f_ss.at[c, m], f_rs.at[c, m],
            device_id={"adapter": partner}, device_id_type=MESH,
        )

    def send_x(m):
        for i in range(1, chips):
            x_copy(i, m).start()

    if near:

        @pl.when(pre)
        def _():
            for p in range(early):
                flow(pre_way, pre_to, pre_slot, 0, p).start()

    for b in range(nb_a):
        if b:
            tok_load(b).wait()
        par_copy(b, 1 - core).start()
        par_copy(b, core).start()

    own_first = lead_core(x) == core

    @pl.when(own_first)
    def _():
        for m in range(nb_a):
            send_x(m)

    def lead_units(lo, hi):
        @pl.when(pre)
        def _():
            def one(p, _):
                lead_unit(p)
                flow(pre_way, pre_to, pre_slot, 0, p).start()
                return 0

            lax.fori_loop(lo, hi, one, 0)

    def from_partner(b):
        par_copy(b, core).wait_recv()

        @pl.when(own_first)
        def _():
            send_x(nb_a + b)

        @pl.when(jnp.logical_not(own_first))
        def _():
            send_x(b)

        par_copy(b, 1 - core).wait_recv()

    def rest_from_partner():
        for b in range(1, nb_a):
            from_partner(b)

        @pl.when(jnp.logical_not(own_first))
        def _():
            for m in range(nb_a, 2 * nb_a):
                send_x(m)

    if near:
        lead_units(early, min(early + 1, np_))
    from_partner(0)
    if near:
        lead_units(min(early + 1, np_), np_)
    dn_load.start()
    up_load.start()
    tables = [
        pltpu.make_async_copy(src, dst, sm_sem.at[i])
        for i, (src, dst) in enumerate(((ids_hbm, ids), (live_hbm, live), (slots_hbm, slots)))
    ]
    for c in tables:
        c.start()
    if not near:
        rest_from_partner()

    def fetch(c, m):
        x_arrival(c, m).wait_recv()
        pass_on(c, m).start()

    def fetched(c, m):
        pass_on(c, m).wait_recv()

    def tell(i, to):
        pl.semaphore_signal(ready.at[i], inc=1, device_id={"tensor": to}, device_id_type=MESH)

    @pl.when(t == 0)
    def _():
        tell(0, right)

    @pl.when(t == T - 1)
    def _():
        tell(1, left)

    def relay():
        @pl.when(jnp.logical_and(t > 0, t < T - 1))
        def _():
            pl.semaphore_wait(ready.at[0], 1)
            tell(0, right)
            pl.semaphore_wait(ready.at[1], 1)
            tell(1, left)

    def all_in():
        @pl.when(t == 0)
        def _():
            pl.semaphore_wait(ready.at[1], 1)

        @pl.when(t == T - 1)
        def _():
            pl.semaphore_wait(ready.at[0], 1)

    def slot_of(k):
        return slots[ids[k]]

    def dn_copy(i):
        to = (a + i) % A
        return pltpu.make_async_remote_copy(
            dn_send.at[to], dn_recv.at[a], dn_ss.at[i], dn_rs.at[i],
            device_id={"adapter": to}, device_id_type=MESH,
        )

    def up_copy(i):
        to = (a + i) % A
        return pltpu.make_async_remote_copy(
            up_send.at[to], up_recv.at[a], up_ss.at[i], up_rs.at[i],
            device_id={"adapter": to}, device_id_type=MESH,
        )

    def s_dest(b):
        k = a * nb_a + b
        return k // nb_t, k % nb_t

    def s_copy(i, b):
        d, kk = s_dest(b)
        return pltpu.make_async_remote_copy(
            s_send.at[b], s_recv.at[t, kk], s_ss.at[i, b], s_rs.at[t, kk],
            device_id={"adapter": (a + i) % A, "tensor": d}, device_id_type=MESH,
        )

    def send_adapters():
        for c in tables:
            c.wait()
        dn_load.wait()
        for i in range(A):
            for b in range(nb_a):
                dn_send[i, b] = dn[lax.rem(slot_of(i * nb_a + b), per_dev)]
        dn_recv[a] = dn_send[a]
        for i in range(1, A):
            dn_copy(i).start()
        up_load.wait()
        for b in range(nb_t):
            sl = lax.rem(slot_of(t * nb_t + b), per_dev)
            for i in range(A):
                up_send[i, b] = up[sl, :, i * cols:(i + 1) * cols]
        up_recv[a] = up_send[a]
        for i in range(1, A):
            up_copy(i).start()

    def send_shrunk():
        all_in()
        for i in range(1, A):
            dn_copy(i).wait_recv()
        for b in range(nb_a):
            k = a * nb_a + b
            mine = dn_recv[lax.div(slot_of(k), per_dev), b]
            s = lax.dot_general(
                mine, tok[k], (((1,), (1,)), ((), ())), preferred_element_type=jnp.float32
            )
            keep = lax.broadcasted_iota(jnp.int32, s.shape, 1) < live[k]
            s_send[b] = jnp.where(keep, s, 0.0).astype(s_send.dtype)
            d, kk = s_dest(b)
            for i in range(A):
                if i:
                    s_copy(i, b).start()
                else:
                    @pl.when(d == t)
                    def _():
                        s_recv[t, kk] = s_send[b]

                    @pl.when(d != t)
                    def _():
                        s_copy(0, b).start()

    def wait_adapters():
        for i in range(1, A):
            up_copy(i).wait_recv()
        for b in range(nb_t):
            owner = (t * nb_t + b) // nb_a
            for tt in range(T):
                c = pltpu.make_async_remote_copy(
                    s_send.at[0], s_recv.at[tt, b], s_ss.at[0, 0], s_rs.at[tt, b],
                    device_id={"adapter": partner}, device_id_type=MESH,
                )

                @pl.when(jnp.logical_or(owner != a, t != tt))
                def _():
                    c.wait_recv()

    remote = [(i, m) for i in range(1, chips) for m in range(2 * nb_a)]
    if not near:
        for i, m in remote:
            fetch((x + i) % chips, m)
        for i, m in remote:
            fetched((x + i) % chips, m)

    units = steps * np_
    if near:
        late = jnp.logical_or(
            jnp.logical_and(t == 0, x == 1), jnp.logical_and(t == T - 1, x == 0)
        )
    lags = (LAG * t, LAG * (T - 1 - t))

    def advance(way, n):
        m = n - lags[way]
        inside = jnp.logical_and(m >= 0, m < units)
        m = jnp.clip(m, 0, units - 1)
        k, p = m // np_, m % np_
        d, h = place(way, k)
        slot = d if way else d - 1
        go = jnp.logical_and(inside, (d < t) if way else (d > t))
        if near:
            go = jnp.logical_and(go, jnp.logical_not(jnp.logical_and(pre, m < np_)))

        @pl.when(go)
        def _():
            mine = base(d * nb_t + h, p)
            fresh = (t == T - 1) if way else (t == 0)

            @pl.when(fresh)
            def _():
                buf[way, slot, h, p] = mine.astype(buf.dtype)

            @pl.when(jnp.logical_not(fresh))
            def _():
                toward(way, slot, h, p).wait_recv()
                buf[way, slot, h, p] = (
                    mine + buf[way, slot, h, p].astype(jnp.float32)
                ).astype(buf.dtype)

            toward(way, slot, h, p).start()

    def iteration(n, _):
        k, p = n // np_, n % np_
        if near:

            @pl.when(n == min(1, np_))
            def _():
                rest_from_partner()

            @pl.when(jnp.logical_and(p == 0, jnp.logical_and(k >= 1, k <= 2 * nb_a)))
            def _():
                def one(m, _):
                    fetch(1 - x, m)
                    fetched(1 - x, m)
                    return 0

                lo = jnp.where(late, jnp.where(k == 2 * nb_a, 0, k), k - 1)
                lax.fori_loop(lo, k, one, 0)

        @pl.when(n == min(1, steps - 1) * np_)
        def _():
            relay()

        @pl.when(n == min(2, steps - 1) * np_)
        def _():
            send_adapters()

        @pl.when(n == max(steps - 2, 0) * np_)
        def _():
            send_shrunk()

        loaded = k == 0
        if near:
            loaded = jnp.logical_and(loaded, jnp.logical_not(pre))

        @pl.when(loaded)
        def _():
            w_load(p).wait()

        advance(0, n)
        advance(1, n)
        h = k - (steps - nb_t)

        @pl.when(jnp.logical_and(h >= 0, h < nb_t))
        def _():
            acc[h, p] = base(t * nb_t + h, p)

        return 0

    lax.fori_loop(0, units + LAG * (T - 2), iteration, 0)
    wait_adapters()
    for b in range(nb_a):
        par_copy(b, 0).wait_send()
        par_copy(b, 1).wait_send()
    for i, m in remote:
        x_copy(i, m).wait_send()
        pass_on((x + i) % chips, m).wait_send()
    for i in range(1, A):
        dn_copy(i).wait_send()
        up_copy(i).wait_send()
    for b in range(nb_a):
        d, _ = s_dest(b)
        for i in range(1, A):
            s_copy(i, b).wait_send()

        @pl.when(d != t)
        def _():
            s_copy(0, b).wait_send()

    def last(n, _):
        h, p = n // np_, n % np_
        own = lax.div(slot_of(t * nb_t + h), per_dev)
        u = up_recv[own, h, :, pl.ds(pl.multiple_of(p * cp, cp), cp)]
        lhs = s_recv[:, h].reshape(T * s_recv.shape[2], BLOCK)
        acc[h, p] = acc[h, p] + SCALE * lax.dot_general(
            lhs, jnp.concatenate([u] * T, axis=0), (((0,), (0,)), ((), ())),
            preferred_element_type=jnp.float32,
        )

        @pl.when(t > 0)
        def _():
            slot = jnp.maximum(t - 1, 0)
            toward(0, slot, h, p).wait_recv()
            acc[h, p] = acc[h, p] + buf[0, slot, h, p].astype(jnp.float32)

        @pl.when(t < T - 1)
        def _():
            slot = jnp.minimum(t, T - 2)
            toward(1, slot, h, p).wait_recv()
            acc[h, p] = acc[h, p] + buf[1, slot, h, p].astype(jnp.float32)

        out_ref[
            pl.ds(pl.multiple_of(h * BLOCK, BLOCK), BLOCK), pl.ds(pl.multiple_of(p * cp, cp), cp)
        ] = acc[h, p].astype(out_ref.dtype)
        return 0

    lax.fori_loop(0, nb_t * np_, last, 0)

    for way in range(2):
        for slot in range(T - 1):

            @pl.when((slot < t) if way else (slot + 1 > t))
            def _():
                pltpu.make_async_remote_copy(
                    buf.at[way, slot], buf.at[way, slot],
                    fl_ss.at[way, slot], fl_rs.at[way, slot, 0, 0],
                    device_id={"tensor": left if way else right}, device_id_type=MESH,
                ).wait_send()


def on_device(tokens, query_weight, down, up, ids, live, slots):
    A, T = lax.axis_size("adapter"), lax.axis_size("tensor")
    rows_a, feat = tokens.shape
    cols = query_weight.shape[1]
    rank = down.shape[1]
    rows_d = rows_a * A // T
    cp = min(512, cols)
    np_ = cols // cp
    nb_a, nb_t = rows_a // BLOCK, rows_d // BLOCK
    chips = A // 2
    bf, f32 = jnp.bfloat16, jnp.float32
    dma = pltpu.SemaphoreType.DMA
    hbm = pl.BlockSpec(memory_space=pl.ANY)
    return pl.pallas_call(
        functools.partial(kernel, A, T),
        out_shape=pltpu.VMEM((rows_d, cols), bf),
        in_specs=[hbm] * 7,
        out_specs=pl.BlockSpec(memory_space=pltpu.VMEM),
        scratch_shapes=[
            pltpu.SMEM(ids.shape, ids.dtype),
            pltpu.SMEM(live.shape, live.dtype),
            pltpu.SMEM(slots.shape, slots.dtype),
            pltpu.VMEM((A * nb_a, BLOCK, feat), bf),
            pltpu.VMEM((np_, feat, cp), bf),
            pltpu.VMEM(down.shape, bf),
            pltpu.VMEM(up.shape, bf),
            pltpu.VMEM((2, T - 1, nb_t, np_, BLOCK, cp), bf),
            pltpu.VMEM((nb_t, np_, BLOCK, cp), f32),
            pltpu.VMEM((A, nb_a, rank, feat), bf),
            pltpu.VMEM((A, nb_a, rank, feat), bf),
            pltpu.VMEM((A, nb_t, rank, cols), bf),
            pltpu.VMEM((A, nb_t, rank, cols), bf),
            pltpu.VMEM((nb_a, rank, BLOCK), bf),
            pltpu.VMEM((T, nb_t, rank, BLOCK), bf),
            dma((3,)), dma((nb_a,)), dma((2,)), dma((np_,)),
            dma((nb_a, 2)), dma((nb_a, 2)),
            dma((chips, 2 * nb_a)), dma((chips, 2 * nb_a)),
            dma((chips, 2 * nb_a)), dma((chips, 2 * nb_a)),
            dma((A,)), dma((A,)), dma((A,)), dma((A,)),
            dma((A, nb_a)), dma((T, nb_t)),
            dma((2, T - 1)), dma((2, T - 1, nb_t, np_)),
            pltpu.SemaphoreType.REGULAR((2,)),
        ],
        compiler_params=pltpu.CompilerParams(
            collective_id=0, has_side_effects=True, vmem_limit_bytes=60 * 1024 * 1024
        ),
    )(ids, live, slots, tokens, query_weight, down, up)


def solution(mesh):
    placed = (
        P(("groups", "adapter"), "tensor"),
        P("tensor", "adapter"),
        P("adapter", None, "tensor"),
        P("adapter", None, None),
        P("groups"),
        P("groups"),
        P("groups"),
    )
    return jax.shard_map(
        on_device,
        mesh=mesh,
        in_specs=placed,
        out_specs=P(("groups", "tensor"), "adapter"),
        check_vma=False,
    )
```

```python
import functools

import jax
import jax.numpy as jnp
from jax import lax
from jax.experimental import pallas as pl
from jax.experimental.pallas import tpu as pltpu
from jax.sharding import PartitionSpec as P

BLOCK = 128
SCALE = 2.0
MESH = pl.DeviceIdType.MESH
PRE = 1
LAG = 3


def kernel(
    A, T,
    ids_hbm, live_hbm, slots_hbm, tok_hbm, w_hbm, dn_hbm, up_hbm, out_ref,
    ids, live, slots, tok, w, dn, up, buf, acc, dn_send, dn_recv, up_send, up_recv,
    s_send, s_col, s_recv,
    sm_sem, ld_sem, w_sem, sent, par_rs, x_rs, f_rs, dn_rs, up_rs,
    col_ss, col_rs, s_ss, s_rs, fl_ss, fl_rs, ready,
):
    a = lax.axis_index("adapter")
    t = lax.axis_index("tensor")
    chips = A // 2
    x, core = a // 2, a % 2
    partner = 2 * x + 1 - core
    nb = tok.shape[0]
    nb_a, nb_t = nb // A, nb // T
    half = BLOCK // 2
    per_dev = dn_hbm.shape[0]
    np_, _, cp = w.shape
    cols = np_ * cp
    steps = (T - 1) * nb_t
    near = chips == 2 and nb_a == nb_t

    def tok_load(b):
        return pltpu.make_async_copy(
            tok_hbm.at[pl.ds(b * BLOCK, BLOCK)], tok.at[a * nb_a + b], ld_sem.at[b]
        )

    def w_load(p):
        c = pl.ds(pl.multiple_of(p * cp, cp), cp)
        return pltpu.make_async_copy(w_hbm.at[:, c], w.at[p], w_sem.at[p])

    dn_load = pltpu.make_async_copy(dn_hbm, dn, ld_sem.at[0])
    up_load = pltpu.make_async_copy(up_hbm, up, ld_sem.at[1])

    tok_load(0).start()
    w_load(0).start()

    barrier = pltpu.get_barrier_semaphore()

    def greet(**to):
        pl.semaphore_signal(barrier, inc=1, device_id=to, device_id_type=MESH)

    @pl.when(t > 0)
    def _():
        greet(tensor=t - 1)

    @pl.when(t < T - 1)
    def _():
        greet(tensor=t + 1)

    for i in range(1, A):
        greet(adapter=(a + i) % A)

    if near:
        lead_r = jnp.where(a >= 1, a, 1)
        lead_l = jnp.where(a <= T - 2, a, T - 2)
        first_r = (T - 1 - lead_r) * nb_t
        first_l = lead_l * nb_t
        pre = jnp.logical_or(
            jnp.logical_and(t == 0, a >= 1), jnp.logical_and(t == T - 1, a <= T - 2)
        )
    else:
        first_r = first_l = 0

    def place(way, k):
        first = first_l if way else first_r
        m = jnp.where(k - 1 < first, k - 1, k)
        m = jnp.where(k == 0, first, m)
        d = m // nb_t
        return (d if way else T - 1 - d), m % nb_t

    def row(way, to, slot):
        return jnp.where(way == 0, slot + 1, jnp.where(slot == to, T, slot))

    def flow(way, to, slot, h, p):
        return pltpu.make_async_remote_copy(
            buf.at[way, slot, h, p], buf.at[way, slot, h, p],
            fl_ss.at[way], fl_rs.at[row(way, to, slot), h, p],
            device_id={"tensor": to}, device_id_type=MESH,
        )

    right, left = (t + 1) % T, (t + T - 1) % T

    def toward(way, slot, h, p):
        return flow(way, left if way else right, slot, h, p)

    def arrival(way, slot, h, p):
        return pltpu.make_async_remote_copy(
            buf.at[way, slot, h, p], buf.at[way, slot, h, p],
            fl_ss.at[way], fl_rs.at[row(way, t, slot), h, p],
            device_id={"tensor": left if way else right}, device_id_type=MESH,
        )

    def base(q, p):
        return jnp.dot(tok[q], w[p], preferred_element_type=jnp.float32)

    early = min(PRE, np_)
    if near:
        pre_way = jnp.where(t == 0, 0, 1)
        pre_slot = jnp.where(t == 0, jnp.maximum(a - 1, 0), jnp.minimum(a, T - 2))
        pre_to = jnp.where(t == 0, 1, T - 2)

    def lead_unit(p):
        w_load(p).wait()
        buf[pre_way, pre_slot, 0, p] = base(a * nb_a, p).astype(buf.dtype)

    tok_load(0).wait()
    for b in range(1, nb_a):
        tok_load(b).start()
    for p in range(1, min(2, np_)):
        w_load(p).start()

    if near:
        @pl.when(pre)
        def _():
            for p in range(early):
                lead_unit(p)

    for p in range(2, np_):
        w_load(p).start()

    ends = jnp.where(t > 0, 1, 0) + jnp.where(t < T - 1, 1, 0)
    pl.semaphore_wait(barrier, A - 1 + ends)

    def par_copy(b, k):
        r = part(a * nb_a + b, k)
        return pltpu.make_async_remote_copy(
            r, r, sent.at[0], par_rs.at[b, k],
            device_id={"adapter": partner}, device_id_type=MESH,
        )

    def lead_core(c):
        return jnp.where(2 * c >= chips, 1, 0)

    def row_block(c, m):
        k = jnp.where(m < nb_a, lead_core(c), 1 - lead_core(c))
        return (2 * c + k) * nb_a + m % nb_a, k

    def part(q, k):
        return tok.at[q, pl.ds(pl.multiple_of(k * half, half), half)]

    def x_copy(i, m):
        r = part(row_block(x, m)[0], core)
        return pltpu.make_async_remote_copy(
            r, r, sent.at[1], x_rs.at[i - 1, m],
            device_id={"adapter": 2 * ((x + i) % chips) + core}, device_id_type=MESH,
        )

    def hop(c):
        return (x - c + chips) % chips - 1

    def x_arrival(c, m):
        r = part(row_block(c, m)[0], core)
        return pltpu.make_async_remote_copy(
            r, r, sent.at[1], x_rs.at[hop(c), m],
            device_id={"adapter": partner}, device_id_type=MESH,
        )

    def pass_on(c, m):
        r = part(row_block(c, m)[0], core)
        return pltpu.make_async_remote_copy(
            r, r, sent.at[2], f_rs.at[hop(c), m],
            device_id={"adapter": partner}, device_id_type=MESH,
        )

    def send_x(m):
        for i in range(1, chips):
            x_copy(i, m).start()

    if near:

        @pl.when(pre)
        def _():
            for p in range(early):
                flow(pre_way, pre_to, pre_slot, 0, p).start()

    for b in range(nb_a):
        if b:
            tok_load(b).wait()
        par_copy(b, 1 - core).start()
        par_copy(b, core).start()

    own_first = lead_core(x) == core

    @pl.when(own_first)
    def _():
        for m in range(nb_a):
            send_x(m)

    def lead_units(lo, hi):
        @pl.when(pre)
        def _():
            def one(p, _):
                lead_unit(p)
                flow(pre_way, pre_to, pre_slot, 0, p).start()
                return 0

            lax.fori_loop(lo, hi, one, 0)

    def from_partner(b):
        par_copy(b, core).wait_recv()

        @pl.when(own_first)
        def _():
            send_x(nb_a + b)

        @pl.when(jnp.logical_not(own_first))
        def _():
            send_x(b)

        par_copy(b, 1 - core).wait_recv()

    def rest_from_partner():
        for b in range(1, nb_a):
            from_partner(b)

        @pl.when(jnp.logical_not(own_first))
        def _():
            for m in range(nb_a, 2 * nb_a):
                send_x(m)

    if near:
        lead_units(early, min(early + 1, np_))
    from_partner(0)
    if near:
        lead_units(min(early + 1, np_), np_)
    dn_load.start()
    up_load.start()
    tables = [
        pltpu.make_async_copy(src, dst, sm_sem.at[i])
        for i, (src, dst) in enumerate(((ids_hbm, ids), (live_hbm, live), (slots_hbm, slots)))
    ]
    for c in tables:
        c.start()
    if not near:
        rest_from_partner()

    def fetch(c, m):
        x_arrival(c, m).wait_recv()
        pass_on(c, m).start()

    def fetched(c, m):
        pass_on(c, m).wait_recv()

    def tell(i, to):
        pl.semaphore_signal(ready.at[i], inc=1, device_id={"tensor": to}, device_id_type=MESH)

    @pl.when(t == 0)
    def _():
        tell(0, right)

    @pl.when(t == T - 1)
    def _():
        tell(1, left)

    def relay():
        @pl.when(jnp.logical_and(t > 0, t < T - 1))
        def _():
            pl.semaphore_wait(ready.at[0], 1)
            tell(0, right)
            pl.semaphore_wait(ready.at[1], 1)
            tell(1, left)

    def all_in():
        @pl.when(t == 0)
        def _():
            pl.semaphore_wait(ready.at[1], 1)

        @pl.when(t == T - 1)
        def _():
            pl.semaphore_wait(ready.at[0], 1)

    def slot_of(k):
        return slots[ids[k]]

    def dn_copy(i):
        to = (a + i) % A
        return pltpu.make_async_remote_copy(
            dn_send.at[to], dn_recv.at[a], sent.at[3], dn_rs.at[0],
            device_id={"adapter": to}, device_id_type=MESH,
        )

    def up_copy(i):
        to = (a + i) % A
        return pltpu.make_async_remote_copy(
            up_send.at[to], up_recv.at[a], sent.at[4], up_rs.at[0],
            device_id={"adapter": to}, device_id_type=MESH,
        )

    def bulk(r, i, recv):
        return pltpu.make_async_remote_copy(
            r, r, sent.at[i], recv, device_id={"adapter": partner}, device_id_type=MESH
        )

    dn_all = bulk(dn_recv.at[pl.ds(0, A - 1)], 3, dn_rs.at[0])
    up_all = bulk(up_recv.at[pl.ds(0, A - 1)], 4, up_rs.at[0])

    def s_dest(b):
        k = a * nb_a + b
        return k // nb_t, k % nb_t

    def col_copy(b):
        return pltpu.make_async_remote_copy(
            s_send.at[b], s_col.at[b, t], col_ss.at[b], col_rs.at[b],
            device_id={"tensor": s_dest(b)[0]}, device_id_type=MESH,
        )

    def s_copy(i, b):
        return pltpu.make_async_remote_copy(
            s_col.at[b], s_recv.at[s_dest(b)[1]], s_ss.at[b], s_rs.at[s_dest(b)[1]],
            device_id={"adapter": (a + i) % A}, device_id_type=MESH,
        )

    def send_adapters():
        for c in tables:
            c.wait()
        dn_load.wait()
        for i in range(A):
            for b in range(nb_a):
                dn_send[i, b] = dn[lax.rem(slot_of(i * nb_a + b), per_dev)]
        dn_recv[a] = dn_send[a]
        for i in range(1, A):
            dn_copy(i).start()
        up_load.wait()
        for b in range(nb_t):
            sl = lax.rem(slot_of(t * nb_t + b), per_dev)
            for i in range(A):
                up_send[i, b] = up[sl, :, i * cols:(i + 1) * cols]
        up_recv[a] = up_send[a]
        for i in range(1, A):
            up_copy(i).start()

    def send_shrunk():
        all_in()
        dn_all.wait_recv()
        for b in range(nb_a):
            k = a * nb_a + b
            mine = dn_recv[lax.div(slot_of(k), per_dev), b]
            s = lax.dot_general(
                mine, tok[k], (((1,), (1,)), ((), ())), preferred_element_type=jnp.float32
            )
            keep = lax.broadcasted_iota(jnp.int32, s.shape, 1) < live[k]
            s_send[b] = jnp.where(keep, s, 0.0).astype(s_send.dtype)
            d, _ = s_dest(b)

            @pl.when(d == t)
            def _():
                s_col[b, t] = s_send[b]

            @pl.when(d != t)
            def _():
                col_copy(b).start()

    def share_shrunk():
        for b in range(nb_a):
            d, kk = s_dest(b)

            @pl.when(d == t)
            def _():
                r = s_col.at[b, pl.ds(0, T - 1)]
                pltpu.make_async_remote_copy(
                    r, r, col_ss.at[b], col_rs.at[b],
                    device_id={"tensor": right}, device_id_type=MESH,
                ).wait_recv()
                for i in range(1, A):
                    s_copy(i, b).start()
                s_recv[kk] = s_col[b]

    def wait_adapters():
        up_all.wait_recv()
        for b in range(nb_t):

            @pl.when((t * nb_t + b) // nb_a != a)
            def _():
                pltpu.make_async_remote_copy(
                    s_recv.at[b], s_recv.at[b], s_ss.at[0], s_rs.at[b],
                    device_id={"adapter": partner}, device_id_type=MESH,
                ).wait_recv()

    remote = [(i, m) for i in range(1, chips) for m in range(2 * nb_a)]
    if not near:
        for i, m in remote:
            fetch((x + i) % chips, m)
        for i, m in remote:
            fetched((x + i) % chips, m)

    units = steps * np_
    if near:
        late = jnp.logical_or(
            jnp.logical_and(t == 0, x == 1), jnp.logical_and(t == T - 1, x == 0)
        )
    lags = (LAG * t, LAG * (T - 1 - t))

    def advance(way, n):
        m = n - lags[way]
        inside = jnp.logical_and(m >= 0, m < units)
        m = jnp.clip(m, 0, units - 1)
        k, p = m // np_, m % np_
        d, h = place(way, k)
        slot = d if way else d - 1
        go = jnp.logical_and(inside, (d < t) if way else (d > t))
        if near:
            go = jnp.logical_and(go, jnp.logical_not(jnp.logical_and(pre, m < np_)))

        @pl.when(go)
        def _():
            mine = base(d * nb_t + h, p)
            fresh = (t == T - 1) if way else (t == 0)

            @pl.when(fresh)
            def _():
                buf[way, slot, h, p] = mine.astype(buf.dtype)

            @pl.when(jnp.logical_not(fresh))
            def _():
                arrival(way, slot, h, p).wait_recv()
                buf[way, slot, h, p] = (
                    mine + buf[way, slot, h, p].astype(jnp.float32)
                ).astype(buf.dtype)

            toward(way, slot, h, p).start()

    def iteration(n, _):
        k, p = n // np_, n % np_
        if near:

            @pl.when(n == min(1, np_))
            def _():
                rest_from_partner()

            @pl.when(jnp.logical_and(p == 0, jnp.logical_and(k >= 1, k <= 2 * nb_a)))
            def _():
                def one(m, _):
                    fetch(1 - x, m)
                    fetched(1 - x, m)
                    return 0

                lo = jnp.where(late, jnp.where(k == 2 * nb_a, 0, k), k - 1)
                lax.fori_loop(lo, k, one, 0)

        @pl.when(n == min(1, steps - 1) * np_)
        def _():
            relay()

        @pl.when(n == min(2, steps - 1) * np_)
        def _():
            send_adapters()

        @pl.when(n == max(steps - 2, 0) * np_)
        def _():
            send_shrunk()

        loaded = k == 0
        if near:
            loaded = jnp.logical_and(loaded, jnp.logical_not(pre))

        @pl.when(loaded)
        def _():
            w_load(p).wait()

        advance(0, n)
        advance(1, n)
        h = k - (steps - nb_t)

        @pl.when(jnp.logical_and(h >= 0, h < nb_t))
        def _():
            acc[h, p] = base(t * nb_t + h, p)

        return 0

    lax.fori_loop(0, units + LAG * (T - 2), iteration, 0)
    share_shrunk()
    wait_adapters()
    bulk(tok.at[pl.ds(0, nb_a)], 0, par_rs.at[0, 0]).wait_send()
    if chips > 1:
        moved = tok.at[pl.ds(0, (chips - 1) * nb_a)]
        bulk(moved, 1, x_rs.at[0, 0]).wait_send()
        bulk(moved, 2, f_rs.at[0, 0]).wait_send()
    dn_all.wait_send()
    up_all.wait_send()
    for b in range(nb_a):
        d, _ = s_dest(b)

        @pl.when(d == t)
        def _():
            r = dn_send.at[pl.ds(0, A - 1), 0, :, pl.ds(0, T * BLOCK)]
            pltpu.make_async_remote_copy(
                r, r, s_ss.at[b], s_rs.at[0],
                device_id={"adapter": partner}, device_id_type=MESH,
            ).wait_send()

        @pl.when(d != t)
        def _():
            col_copy(b).wait_send()

    def last(n, _):
        h, p = n // np_, n % np_
        own = lax.div(slot_of(t * nb_t + h), per_dev)
        u = up_recv[own, h, :, pl.ds(pl.multiple_of(p * cp, cp), cp)]
        lhs = s_recv[h].reshape(T * s_recv.shape[2], BLOCK)
        acc[h, p] = acc[h, p] + SCALE * lax.dot_general(
            lhs, jnp.concatenate([u] * T, axis=0), (((0,), (0,)), ((), ())),
            preferred_element_type=jnp.float32,
        )

        @pl.when(t > 0)
        def _():
            slot = jnp.maximum(t - 1, 0)
            arrival(0, slot, h, p).wait_recv()
            acc[h, p] = acc[h, p] + buf[0, slot, h, p].astype(jnp.float32)

        @pl.when(t < T - 1)
        def _():
            slot = jnp.minimum(t, T - 2)
            arrival(1, slot, h, p).wait_recv()
            acc[h, p] = acc[h, p] + buf[1, slot, h, p].astype(jnp.float32)

        out_ref[
            pl.ds(pl.multiple_of(h * BLOCK, BLOCK), BLOCK), pl.ds(pl.multiple_of(p * cp, cp), cp)
        ] = acc[h, p].astype(out_ref.dtype)
        return 0

    lax.fori_loop(0, nb_t * np_, last, 0)

    def drain(way, count):
        r = buf.at[way, pl.ds(0, count)]
        pltpu.make_async_remote_copy(
            r, r, fl_ss.at[way], fl_rs.at[0, 0, 0],
            device_id={"tensor": left if way else right}, device_id_type=MESH,
        ).wait_send()

    for i in range(T):

        @pl.when(t == i)
        def _():
            if i < T - 1:
                drain(0, T - 1 - i)
            if i > 0:
                drain(1, i)


def on_device(tokens, query_weight, down, up, ids, live, slots):
    A, T = lax.axis_size("adapter"), lax.axis_size("tensor")
    rows_a, feat = tokens.shape
    cols = query_weight.shape[1]
    rank = down.shape[1]
    rows_d = rows_a * A // T
    cp = min(512, cols)
    np_ = cols // cp
    nb_a, nb_t = rows_a // BLOCK, rows_d // BLOCK
    chips = A // 2
    bf, f32 = jnp.bfloat16, jnp.float32
    dma = pltpu.SemaphoreType.DMA
    hbm = pl.BlockSpec(memory_space=pl.ANY)
    return pl.pallas_call(
        functools.partial(kernel, A, T),
        out_shape=pltpu.VMEM((rows_d, cols), bf),
        in_specs=[hbm] * 7,
        out_specs=pl.BlockSpec(memory_space=pltpu.VMEM),
        scratch_shapes=[
            pltpu.SMEM(ids.shape, ids.dtype),
            pltpu.SMEM(live.shape, live.dtype),
            pltpu.SMEM(slots.shape, slots.dtype),
            pltpu.VMEM((A * nb_a, BLOCK, feat), bf),
            pltpu.VMEM((np_, feat, cp), bf),
            pltpu.VMEM(down.shape, bf),
            pltpu.VMEM(up.shape, bf),
            pltpu.VMEM((2, T - 1, nb_t, np_, BLOCK, cp), bf),
            pltpu.VMEM((nb_t, np_, BLOCK, cp), f32),
            pltpu.VMEM((A, nb_a, rank, feat), bf),
            pltpu.VMEM((A, nb_a, rank, feat), bf),
            pltpu.VMEM((A, nb_t, rank, cols), bf),
            pltpu.VMEM((A, nb_t, rank, cols), bf),
            pltpu.VMEM((nb_a, rank, BLOCK), bf),
            pltpu.VMEM((nb_a, T, rank, BLOCK), bf),
            pltpu.VMEM((nb_t, T, rank, BLOCK), bf),
            dma((3,)), dma((max(nb_a, 2),)), dma((np_,)), dma((5,)),
            dma((nb_a, 2)), dma((max(chips - 1, 1), 2 * nb_a)), dma((max(chips - 1, 1), 2 * nb_a)),
            dma((1,)), dma((1,)),
            dma((nb_a,)), dma((nb_a,)), dma((nb_a,)), dma((nb_t,)),
            dma((2,)), dma((T + 1, nb_t, np_)),
            pltpu.SemaphoreType.REGULAR((2,)),
        ],
        compiler_params=pltpu.CompilerParams(
            collective_id=0, has_side_effects=True, vmem_limit_bytes=60 * 1024 * 1024
        ),
    )(ids, live, slots, tokens, query_weight, down, up)


def solution(mesh):
    placed = (
        P(("groups", "adapter"), "tensor"),
        P("tensor", "adapter"),
        P("adapter", None, "tensor"),
        P("adapter", None, None),
        P("groups"),
        P("groups"),
        P("groups"),
    )
    return jax.shard_map(
        on_device,
        mesh=mesh,
        in_specs=placed,
        out_specs=P(("groups", "tensor"), "adapter"),
        check_vma=False,
    )
```

```python
import functools

import jax
import jax.numpy as jnp
from jax import lax
from jax.experimental import pallas as pl
from jax.experimental.pallas import tpu as pltpu
from jax.sharding import PartitionSpec as P

BLOCK = 128
SCALE = 2.0
MESH = pl.DeviceIdType.MESH
PRE = 1
LAG = 3


def kernel(
    A, T,
    ids_hbm, live_hbm, slots_hbm, tok_hbm, w_hbm, dn_hbm, up_hbm, out_ref,
    ids, live, slots, tok, w, dn, up, buf, acc, dn_send, dn_recv, up_send, up_recv,
    s_send, s_col, s_recv,
    sm_sem, ld_sem, w_sem, sent, par_rs, x_rs, f_rs, dn_rs, up_rs,
    col_ss, col_rs, s_ss, s_rs, fl_ss, fl_rs, ready,
):
    a = lax.axis_index("adapter")
    t = lax.axis_index("tensor")
    chips = A // 2
    x, core = a // 2, a % 2
    partner = 2 * x + 1 - core
    nb = tok.shape[0]
    nb_a, nb_t = nb // A, nb // T
    half = BLOCK // 2
    per_dev = dn_hbm.shape[0]
    np_, _, cp = w.shape
    cols = np_ * cp
    steps = (T - 1) * nb_t
    near = chips == 2 and nb_a == nb_t

    def tok_load(b):
        return pltpu.make_async_copy(
            tok_hbm.at[pl.ds(b * BLOCK, BLOCK)], tok.at[a * nb_a + b], ld_sem.at[b]
        )

    def w_load(p):
        c = pl.ds(pl.multiple_of(p * cp, cp), cp)
        return pltpu.make_async_copy(w_hbm.at[:, c], w.at[p], w_sem.at[p])

    dn_load = pltpu.make_async_copy(dn_hbm, dn, ld_sem.at[0])
    up_load = pltpu.make_async_copy(up_hbm, up, ld_sem.at[1])

    tok_load(0).start()
    w_load(0).start()

    barrier = pltpu.get_barrier_semaphore()

    def greet(**to):
        pl.semaphore_signal(barrier, inc=1, device_id=to, device_id_type=MESH)

    @pl.when(t > 0)
    def _():
        greet(tensor=t - 1)

    @pl.when(t < T - 1)
    def _():
        greet(tensor=t + 1)

    for i in range(1, A):
        greet(adapter=(a + i) % A)

    if near:
        lead_r = jnp.where(a >= 1, a, 1)
        lead_l = jnp.where(a <= T - 2, a, T - 2)
        first_r = (T - 1 - lead_r) * nb_t
        first_l = lead_l * nb_t
        pre = jnp.logical_or(
            jnp.logical_and(t == 0, a >= 1), jnp.logical_and(t == T - 1, a <= T - 2)
        )
    else:
        first_r = first_l = 0

    def place(way, k):
        first = first_l if way else first_r
        m = jnp.where(k - 1 < first, k - 1, k)
        m = jnp.where(k == 0, first, m)
        d = m // nb_t
        return (d if way else T - 1 - d), m % nb_t

    def row(way, to, slot):
        return jnp.where(way == 0, slot + 1, jnp.where(slot == to, T, slot))

    def flow(way, to, slot, h, p):
        return pltpu.make_async_remote_copy(
            buf.at[way, slot, h, p], buf.at[way, slot, h, p],
            fl_ss.at[way], fl_rs.at[row(way, to, slot), h, p],
            device_id={"tensor": to}, device_id_type=MESH,
        )

    right, left = (t + 1) % T, (t + T - 1) % T

    def toward(way, slot, h, p):
        return flow(way, left if way else right, slot, h, p)

    def arrival(way, slot, h, p):
        return pltpu.make_async_remote_copy(
            buf.at[way, slot, h, p], buf.at[way, slot, h, p],
            fl_ss.at[way], fl_rs.at[row(way, t, slot), h, p],
            device_id={"tensor": left if way else right}, device_id_type=MESH,
        )

    def base(q, p):
        return jnp.dot(tok[q], w[p], preferred_element_type=jnp.float32)

    early = min(PRE, np_)
    if near:
        pre_way = jnp.where(t == 0, 0, 1)
        pre_slot = jnp.where(t == 0, jnp.maximum(a - 1, 0), jnp.minimum(a, T - 2))
        pre_to = jnp.where(t == 0, 1, T - 2)

    def lead_unit(p):
        w_load(p).wait()
        buf[pre_way, pre_slot, 0, p] = base(a * nb_a, p).astype(buf.dtype)

    for p in range(1, min(2, np_)):
        w_load(p).start()
    tok_load(0).wait()
    for b in range(1, nb_a):
        tok_load(b).start()
    if near:
        @pl.when(pre)
        def _():
            for p in range(early):
                lead_unit(p)

    ends = jnp.where(t > 0, 1, 0) + jnp.where(t < T - 1, 1, 0)
    pl.semaphore_wait(barrier, A - 1 + ends)

    def par_copy(b, k):
        r = part(a * nb_a + b, k)
        return pltpu.make_async_remote_copy(
            r, r, sent.at[0], par_rs.at[b, k],
            device_id={"adapter": partner}, device_id_type=MESH,
        )

    def lead_core(c):
        return jnp.where(2 * c >= chips, 1, 0)

    def row_block(c, m):
        k = jnp.where(m < nb_a, lead_core(c), 1 - lead_core(c))
        return (2 * c + k) * nb_a + m % nb_a, k

    def part(q, k):
        return tok.at[q, pl.ds(pl.multiple_of(k * half, half), half)]

    def x_copy(i, m):
        r = part(row_block(x, m)[0], core)
        return pltpu.make_async_remote_copy(
            r, r, sent.at[1], x_rs.at[i - 1, m],
            device_id={"adapter": 2 * ((x + i) % chips) + core}, device_id_type=MESH,
        )

    def hop(c):
        return (x - c + chips) % chips - 1

    def x_arrival(c, m):
        r = part(row_block(c, m)[0], core)
        return pltpu.make_async_remote_copy(
            r, r, sent.at[1], x_rs.at[hop(c), m],
            device_id={"adapter": partner}, device_id_type=MESH,
        )

    def pass_on(c, m):
        r = part(row_block(c, m)[0], core)
        return pltpu.make_async_remote_copy(
            r, r, sent.at[2], f_rs.at[hop(c), m],
            device_id={"adapter": partner}, device_id_type=MESH,
        )

    def send_x(m):
        for i in range(1, chips):
            x_copy(i, m).start()

    if near:

        @pl.when(pre)
        def _():
            for p in range(early):
                flow(pre_way, pre_to, pre_slot, 0, p).start()

    for b in range(nb_a):
        if b:
            tok_load(b).wait()
        par_copy(b, 1 - core).start()
        par_copy(b, core).start()

    own_first = lead_core(x) == core

    @pl.when(own_first)
    def _():
        for m in range(nb_a):
            send_x(m)

    def lead_units(lo, hi):
        @pl.when(pre)
        def _():
            def one(p, _):
                lead_unit(p)
                flow(pre_way, pre_to, pre_slot, 0, p).start()
                return 0

            lax.fori_loop(lo, hi, one, 0)

    def from_partner(b):
        par_copy(b, core).wait_recv()

        @pl.when(own_first)
        def _():
            send_x(nb_a + b)

        @pl.when(jnp.logical_not(own_first))
        def _():
            send_x(b)

        par_copy(b, 1 - core).wait_recv()

    def rest_from_partner():
        for b in range(1, nb_a):
            from_partner(b)

        @pl.when(jnp.logical_not(own_first))
        def _():
            for m in range(nb_a, 2 * nb_a):
                send_x(m)

    if near:
        lead_units(early, min(early + 1, np_))
    for p in range(2, np_):
        w_load(p).start()
    from_partner(0)
    if near:
        lead_units(min(early + 1, np_), np_)
    tables = [
        pltpu.make_async_copy(src, dst, sm_sem.at[i])
        for i, (src, dst) in enumerate(((ids_hbm, ids), (live_hbm, live), (slots_hbm, slots)))
    ]
    if not near:
        rest_from_partner()

    def fetch(c, m):
        x_arrival(c, m).wait_recv()
        pass_on(c, m).start()

    def fetched(c, m):
        pass_on(c, m).wait_recv()

    def tell(i, to):
        pl.semaphore_signal(ready.at[i], inc=1, device_id={"tensor": to}, device_id_type=MESH)

    @pl.when(t == 0)
    def _():
        tell(0, right)

    @pl.when(t == T - 1)
    def _():
        tell(1, left)

    def relay():
        @pl.when(jnp.logical_and(t > 0, t < T - 1))
        def _():
            pl.semaphore_wait(ready.at[0], 1)
            tell(0, right)
            pl.semaphore_wait(ready.at[1], 1)
            tell(1, left)

    def all_in():
        @pl.when(t == 0)
        def _():
            pl.semaphore_wait(ready.at[1], 1)

        @pl.when(t == T - 1)
        def _():
            pl.semaphore_wait(ready.at[0], 1)

    def slot_of(k):
        return slots[ids[k]]

    def dn_copy(i):
        to = (a + i) % A
        return pltpu.make_async_remote_copy(
            dn_send.at[to], dn_recv.at[a], sent.at[3], dn_rs.at[0],
            device_id={"adapter": to}, device_id_type=MESH,
        )

    def up_copy(i):
        to = (a + i) % A
        return pltpu.make_async_remote_copy(
            up_send.at[to], up_recv.at[a], sent.at[4], up_rs.at[0],
            device_id={"adapter": to}, device_id_type=MESH,
        )

    def bulk(r, i, recv):
        return pltpu.make_async_remote_copy(
            r, r, sent.at[i], recv, device_id={"adapter": partner}, device_id_type=MESH
        )

    dn_all = bulk(dn_recv.at[pl.ds(0, A - 1)], 3, dn_rs.at[0])
    up_all = bulk(up_recv.at[pl.ds(0, A - 1)], 4, up_rs.at[0])

    def s_dest(b):
        k = a * nb_a + b
        return k // nb_t, k % nb_t

    def col_copy(b):
        return pltpu.make_async_remote_copy(
            s_send.at[b], s_col.at[b, t], col_ss.at[b], col_rs.at[b],
            device_id={"tensor": s_dest(b)[0]}, device_id_type=MESH,
        )

    def s_copy(i, b):
        return pltpu.make_async_remote_copy(
            s_col.at[b], s_recv.at[s_dest(b)[1]], s_ss.at[b], s_rs.at[s_dest(b)[1]],
            device_id={"adapter": (a + i) % A}, device_id_type=MESH,
        )

    def send_adapters():
        for c in tables:
            c.wait()
        dn_load.wait()
        for i in range(A):
            for b in range(nb_a):
                dn_send[i, b] = dn[lax.rem(slot_of(i * nb_a + b), per_dev)]
        dn_recv[a] = dn_send[a]
        for i in range(1, A):
            dn_copy(i).start()
        up_load.wait()
        for b in range(nb_t):
            sl = lax.rem(slot_of(t * nb_t + b), per_dev)
            for i in range(A):
                up_send[i, b] = up[sl, :, i * cols:(i + 1) * cols]
        up_recv[a] = up_send[a]
        for i in range(1, A):
            up_copy(i).start()

    def send_shrunk():
        all_in()
        dn_all.wait_recv()
        for b in range(nb_a):
            k = a * nb_a + b
            mine = dn_recv[lax.div(slot_of(k), per_dev), b]
            s = lax.dot_general(
                mine, tok[k], (((1,), (1,)), ((), ())), preferred_element_type=jnp.float32
            )
            keep = lax.broadcasted_iota(jnp.int32, s.shape, 1) < live[k]
            s_send[b] = jnp.where(keep, s, 0.0).astype(s_send.dtype)
            d, _ = s_dest(b)

            @pl.when(d == t)
            def _():
                s_col[b, t] = s_send[b]

            @pl.when(d != t)
            def _():
                col_copy(b).start()

    def share_shrunk():
        for b in range(nb_a):
            d, kk = s_dest(b)

            @pl.when(d == t)
            def _():
                r = s_col.at[b, pl.ds(0, T - 1)]
                pltpu.make_async_remote_copy(
                    r, r, col_ss.at[b], col_rs.at[b],
                    device_id={"tensor": right}, device_id_type=MESH,
                ).wait_recv()
                for i in range(1, A):
                    s_copy(i, b).start()
                s_recv[kk] = s_col[b]

    def wait_adapters():
        up_all.wait_recv()
        for b in range(nb_t):

            @pl.when((t * nb_t + b) // nb_a != a)
            def _():
                pltpu.make_async_remote_copy(
                    s_recv.at[b], s_recv.at[b], s_ss.at[0], s_rs.at[b],
                    device_id={"adapter": partner}, device_id_type=MESH,
                ).wait_recv()

    remote = [(i, m) for i in range(1, chips) for m in range(2 * nb_a)]
    if not near:
        for i, m in remote:
            fetch((x + i) % chips, m)
        for i, m in remote:
            fetched((x + i) % chips, m)

    units = steps * np_
    if near:
        late = jnp.logical_or(
            jnp.logical_and(t == 0, x == 1), jnp.logical_and(t == T - 1, x == 0)
        )
    lags = (LAG * t, LAG * (T - 1 - t))

    def advance(way, n):
        m = n - lags[way]
        inside = jnp.logical_and(m >= 0, m < units)
        m = jnp.clip(m, 0, units - 1)
        k, p = m // np_, m % np_
        d, h = place(way, k)
        slot = d if way else d - 1
        go = jnp.logical_and(inside, (d < t) if way else (d > t))
        if near:
            go = jnp.logical_and(go, jnp.logical_not(jnp.logical_and(pre, m < np_)))

        @pl.when(go)
        def _():
            mine = base(d * nb_t + h, p)
            fresh = (t == T - 1) if way else (t == 0)

            @pl.when(fresh)
            def _():
                buf[way, slot, h, p] = mine.astype(buf.dtype)

            @pl.when(jnp.logical_not(fresh))
            def _():
                arrival(way, slot, h, p).wait_recv()
                buf[way, slot, h, p] = (
                    mine + buf[way, slot, h, p].astype(jnp.float32)
                ).astype(buf.dtype)

            toward(way, slot, h, p).start()

    def iteration(n, _):
        k, p = n // np_, n % np_
        if near:

            @pl.when(n == min(1, np_))
            def _():
                rest_from_partner()

            @pl.when(jnp.logical_and(p == 0, jnp.logical_and(k >= 1, k <= 2 * nb_a)))
            def _():
                def one(m, _):
                    fetch(1 - x, m)
                    fetched(1 - x, m)
                    return 0

                lo = jnp.where(late, jnp.where(k == 2 * nb_a, 0, k), k - 1)
                lax.fori_loop(lo, k, one, 0)

        @pl.when(n == min(1, steps - 1) * np_)
        def _():
            for c in tables + [dn_load, up_load]:
                c.start()
            relay()

        @pl.when(n == min(2, steps - 1) * np_)
        def _():
            send_adapters()

        @pl.when(n == max(steps - 2, 0) * np_)
        def _():
            send_shrunk()

        loaded = k == 0
        if near:
            loaded = jnp.logical_and(loaded, jnp.logical_not(pre))

        @pl.when(loaded)
        def _():
            w_load(p).wait()

        advance(0, n)
        advance(1, n)
        h = k - (steps - nb_t)

        @pl.when(jnp.logical_and(h >= 0, h < nb_t))
        def _():
            acc[h, p] = base(t * nb_t + h, p)

        return 0

    lax.fori_loop(0, units + LAG * (T - 2), iteration, 0)
    share_shrunk()
    wait_adapters()
    bulk(tok.at[pl.ds(0, nb_a)], 0, par_rs.at[0, 0]).wait_send()
    if chips > 1:
        moved = tok.at[pl.ds(0, (chips - 1) * nb_a)]
        bulk(moved, 1, x_rs.at[0, 0]).wait_send()
        bulk(moved, 2, f_rs.at[0, 0]).wait_send()
    dn_all.wait_send()
    up_all.wait_send()
    for b in range(nb_a):
        d, _ = s_dest(b)

        @pl.when(d == t)
        def _():
            r = dn_send.at[pl.ds(0, A - 1), 0, :, pl.ds(0, T * BLOCK)]
            pltpu.make_async_remote_copy(
                r, r, s_ss.at[b], s_rs.at[0],
                device_id={"adapter": partner}, device_id_type=MESH,
            ).wait_send()

        @pl.when(d != t)
        def _():
            col_copy(b).wait_send()

    def last(n, _):
        h, p = n // np_, n % np_
        own = lax.div(slot_of(t * nb_t + h), per_dev)
        u = up_recv[own, h, :, pl.ds(pl.multiple_of(p * cp, cp), cp)]
        lhs = s_recv[h].reshape(T * s_recv.shape[2], BLOCK)
        acc[h, p] = acc[h, p] + SCALE * lax.dot_general(
            lhs, jnp.concatenate([u] * T, axis=0), (((0,), (0,)), ((), ())),
            preferred_element_type=jnp.float32,
        )

        @pl.when(t > 0)
        def _():
            slot = jnp.maximum(t - 1, 0)
            arrival(0, slot, h, p).wait_recv()
            acc[h, p] = acc[h, p] + buf[0, slot, h, p].astype(jnp.float32)

        @pl.when(t < T - 1)
        def _():
            slot = jnp.minimum(t, T - 2)
            arrival(1, slot, h, p).wait_recv()
            acc[h, p] = acc[h, p] + buf[1, slot, h, p].astype(jnp.float32)

        out_ref[
            pl.ds(pl.multiple_of(h * BLOCK, BLOCK), BLOCK), pl.ds(pl.multiple_of(p * cp, cp), cp)
        ] = acc[h, p].astype(out_ref.dtype)
        return 0

    lax.fori_loop(0, nb_t * np_, last, 0)

    def drain(way, count):
        r = buf.at[way, pl.ds(0, count)]
        pltpu.make_async_remote_copy(
            r, r, fl_ss.at[way], fl_rs.at[0, 0, 0],
            device_id={"tensor": left if way else right}, device_id_type=MESH,
        ).wait_send()

    for i in range(T):

        @pl.when(t == i)
        def _():
            if i < T - 1:
                drain(0, T - 1 - i)
            if i > 0:
                drain(1, i)


def on_device(tokens, query_weight, down, up, ids, live, slots):
    A, T = lax.axis_size("adapter"), lax.axis_size("tensor")
    rows_a, feat = tokens.shape
    cols = query_weight.shape[1]
    rank = down.shape[1]
    rows_d = rows_a * A // T
    cp = min(512, cols)
    np_ = cols // cp
    nb_a, nb_t = rows_a // BLOCK, rows_d // BLOCK
    chips = A // 2
    bf, f32 = jnp.bfloat16, jnp.float32
    dma = pltpu.SemaphoreType.DMA
    hbm = pl.BlockSpec(memory_space=pl.ANY)
    return pl.pallas_call(
        functools.partial(kernel, A, T),
        out_shape=pltpu.VMEM((rows_d, cols), bf),
        in_specs=[hbm] * 7,
        out_specs=pl.BlockSpec(memory_space=pltpu.VMEM),
        scratch_shapes=[
            pltpu.SMEM(ids.shape, ids.dtype),
            pltpu.SMEM(live.shape, live.dtype),
            pltpu.SMEM(slots.shape, slots.dtype),
            pltpu.VMEM((A * nb_a, BLOCK, feat), bf),
            pltpu.VMEM((np_, feat, cp), bf),
            pltpu.VMEM(down.shape, bf),
            pltpu.VMEM(up.shape, bf),
            pltpu.VMEM((2, T - 1, nb_t, np_, BLOCK, cp), bf),
            pltpu.VMEM((nb_t, np_, BLOCK, cp), f32),
            pltpu.VMEM((A, nb_a, rank, feat), bf),
            pltpu.VMEM((A, nb_a, rank, feat), bf),
            pltpu.VMEM((A, nb_t, rank, cols), bf),
            pltpu.VMEM((A, nb_t, rank, cols), bf),
            pltpu.VMEM((nb_a, rank, BLOCK), bf),
            pltpu.VMEM((nb_a, T, rank, BLOCK), bf),
            pltpu.VMEM((nb_t, T, rank, BLOCK), bf),
            dma((3,)), dma((max(nb_a, 2),)), dma((np_,)), dma((5,)),
            dma((nb_a, 2)), dma((max(chips - 1, 1), 2 * nb_a)), dma((max(chips - 1, 1), 2 * nb_a)),
            dma((1,)), dma((1,)),
            dma((nb_a,)), dma((nb_a,)), dma((nb_a,)), dma((nb_t,)),
            dma((2,)), dma((T + 1, nb_t, np_)),
            pltpu.SemaphoreType.REGULAR((2,)),
        ],
        compiler_params=pltpu.CompilerParams(
            collective_id=0, has_side_effects=True, vmem_limit_bytes=60 * 1024 * 1024
        ),
    )(ids, live, slots, tokens, query_weight, down, up)


def solution(mesh):
    placed = (
        P(("groups", "adapter"), "tensor"),
        P("tensor", "adapter"),
        P("adapter", None, "tensor"),
        P("adapter", None, None),
        P("groups"),
        P("groups"),
        P("groups"),
    )
    return jax.shard_map(
        on_device,
        mesh=mesh,
        in_specs=placed,
        out_specs=P(("groups", "tensor"), "adapter"),
        check_vma=False,
    )
```

```python
import functools

import jax
import jax.numpy as jnp
from jax import lax
from jax.experimental import pallas as pl
from jax.experimental.pallas import tpu as pltpu
from jax.sharding import PartitionSpec as P

BLOCK = 128
SCALE = 2.0
MESH = pl.DeviceIdType.MESH
LAG = 3


def kernel(
    A, T,
    ids_hbm, live_hbm, slots_hbm, tok_hbm, w_hbm, dn_hbm, up_hbm, out_ref,
    ids, live, slots, tok, w, dn, up, buf, acc, dn_send, dn_recv, up_send, up_recv,
    s_send, s_col, s_recv,
    sm_sem, ld_sem, w_sem, sent, par_rs, x_rs, f_rs, dn_rs, up_rs,
    col_ss, col_rs, s_ss, s_rs, fl_ss, fl_rs, ready,
):
    a = lax.axis_index("adapter")
    t = lax.axis_index("tensor")
    chips = A // 2
    x, core = a // 2, a % 2
    partner = 2 * x + 1 - core
    nb = tok.shape[0]
    nb_a, nb_t = nb // A, nb // T
    half = BLOCK // 2
    per_dev = dn_hbm.shape[0]
    np_, _, cp = w.shape
    cols = np_ * cp
    steps = (T - 1) * nb_t
    near = chips == 2 and nb_a == nb_t

    def tok_load(b):
        return pltpu.make_async_copy(
            tok_hbm.at[pl.ds(b * BLOCK, BLOCK)], tok.at[a * nb_a + b], ld_sem.at[b]
        )

    piece = cp // 2 if cp % 256 == 0 else cp
    pieces = cp // piece

    def w_piece(i):
        c = pl.ds(i * piece, piece)
        return pltpu.make_async_copy(
            w_hbm.at[:, c], w.at[0, :, c], w_sem.at[np_ if i else 0]
        )

    def w_load(p):
        c = pl.ds(pl.multiple_of(p * cp, cp), cp)
        return pltpu.make_async_copy(w_hbm.at[:, c], w.at[p], w_sem.at[p])

    dn_load = pltpu.make_async_copy(dn_hbm, dn, ld_sem.at[0])
    up_load = pltpu.make_async_copy(up_hbm, up, ld_sem.at[1])

    tok_load(0).start()
    w_piece(0).start()

    barrier = pltpu.get_barrier_semaphore()

    def greet(**to):
        pl.semaphore_signal(barrier, inc=1, device_id=to, device_id_type=MESH)

    @pl.when(t > 0)
    def _():
        greet(tensor=t - 1)

    @pl.when(t < T - 1)
    def _():
        greet(tensor=t + 1)

    for i in range(1, A):
        greet(adapter=(a + i) % A)

    if near:
        lead_r = jnp.where(a >= 1, a, 1)
        lead_l = jnp.where(a <= T - 2, a, T - 2)
        first_r = (T - 1 - lead_r) * nb_t
        first_l = lead_l * nb_t
        pre = jnp.logical_or(
            jnp.logical_and(t == 0, a >= 1), jnp.logical_and(t == T - 1, a <= T - 2)
        )
    else:
        first_r = first_l = 0

    def place(way, k):
        first = first_l if way else first_r
        m = jnp.where(k - 1 < first, k - 1, k)
        m = jnp.where(k == 0, first, m)
        d = m // nb_t
        return (d if way else T - 1 - d), m % nb_t

    def row(way, to, slot):
        return jnp.where(way == 0, slot + 1, jnp.where(slot == to, T, slot))

    def flow(way, to, slot, h, p):
        return pltpu.make_async_remote_copy(
            buf.at[way, slot, h, p], buf.at[way, slot, h, p],
            fl_ss.at[way], fl_rs.at[row(way, to, slot), h, p],
            device_id={"tensor": to}, device_id_type=MESH,
        )

    right, left = (t + 1) % T, (t + T - 1) % T

    def toward(way, slot, h, p):
        return flow(way, left if way else right, slot, h, p)

    def arrival(way, slot, h, p):
        return pltpu.make_async_remote_copy(
            buf.at[way, slot, h, p], buf.at[way, slot, h, p],
            fl_ss.at[way], fl_rs.at[row(way, t, slot), h, p],
            device_id={"tensor": left if way else right}, device_id_type=MESH,
        )

    def base(q, p):
        return jnp.dot(tok[q], w[p], preferred_element_type=jnp.float32)

    if near:
        pre_way = jnp.where(t == 0, 0, 1)
        pre_slot = jnp.where(t == 0, jnp.maximum(a - 1, 0), jnp.minimum(a, T - 2))
        pre_to = jnp.where(t == 0, 1, T - 2)

    def lead_unit(p):
        w_load(p).wait()
        buf[pre_way, pre_slot, 0, p] = base(a * nb_a, p).astype(buf.dtype)

    def lead_piece(i):
        w_piece(i).wait()
        c = slice(i * piece, (i + 1) * piece)
        buf[pre_way, pre_slot, 0, 0, :, c] = jnp.dot(
            tok[a * nb_a], w[0, :, c], preferred_element_type=jnp.float32
        ).astype(buf.dtype)

    def send_piece(i):
        r = buf.at[pre_way, pre_slot, 0, 0, :, pl.ds(i * piece, piece)]
        pltpu.make_async_remote_copy(
            r, r, fl_ss.at[pre_way], fl_rs.at[row(pre_way, pre_to, pre_slot), 0, 0],
            device_id={"tensor": pre_to}, device_id_type=MESH,
        ).start()

    for i in range(1, pieces):
        w_piece(i).start()
    for b in range(1, nb_a):
        tok_load(b).start()
    for p in range(1, min(2, np_)):
        w_load(p).start()
    tok_load(0).wait()
    if near:
        @pl.when(pre)
        def _():
            lead_piece(0)

        @pl.when(jnp.logical_and(pre, t == 0))
        def _():
            for i in range(1, pieces):
                lead_piece(i)

    for p in range(2, np_):
        w_load(p).start()

    ends = jnp.where(t > 0, 1, 0) + jnp.where(t < T - 1, 1, 0)
    pl.semaphore_wait(barrier, A - 1 + ends)

    def par_copy(b, k):
        r = part(a * nb_a + b, k)
        return pltpu.make_async_remote_copy(
            r, r, sent.at[0], par_rs.at[b, k],
            device_id={"adapter": partner}, device_id_type=MESH,
        )

    def lead_core(c):
        return jnp.where(2 * c >= chips, 1, 0)

    def row_block(c, m):
        k = jnp.where(m < nb_a, lead_core(c), 1 - lead_core(c))
        return (2 * c + k) * nb_a + m % nb_a, k

    def part(q, k):
        return tok.at[q, pl.ds(pl.multiple_of(k * half, half), half)]

    def x_copy(i, m):
        r = part(row_block(x, m)[0], core)
        return pltpu.make_async_remote_copy(
            r, r, sent.at[1], x_rs.at[i - 1, m],
            device_id={"adapter": 2 * ((x + i) % chips) + core}, device_id_type=MESH,
        )

    def hop(c):
        return (x - c + chips) % chips - 1

    def x_arrival(c, m):
        r = part(row_block(c, m)[0], core)
        return pltpu.make_async_remote_copy(
            r, r, sent.at[1], x_rs.at[hop(c), m],
            device_id={"adapter": partner}, device_id_type=MESH,
        )

    def pass_on(c, m):
        r = part(row_block(c, m)[0], core)
        return pltpu.make_async_remote_copy(
            r, r, sent.at[2], f_rs.at[hop(c), m],
            device_id={"adapter": partner}, device_id_type=MESH,
        )

    def send_x(m):
        for i in range(1, chips):
            x_copy(i, m).start()

    if near:

        @pl.when(pre)
        def _():
            send_piece(0)

        @pl.when(jnp.logical_and(pre, t == 0))
        def _():
            for i in range(1, pieces):
                send_piece(i)

    for b in range(nb_a):
        if b:
            tok_load(b).wait()
        par_copy(b, 1 - core).start()
        par_copy(b, core).start()

    own_first = lead_core(x) == core

    @pl.when(own_first)
    def _():
        for m in range(nb_a):
            send_x(m)

    def lead_units(lo, hi):
        @pl.when(pre)
        def _():
            def one(p, _):
                lead_unit(p)
                flow(pre_way, pre_to, pre_slot, 0, p).start()
                return 0

            lax.fori_loop(lo, hi, one, 0)

    def from_partner(b):
        par_copy(b, core).wait_recv()

        @pl.when(own_first)
        def _():
            send_x(nb_a + b)

        @pl.when(jnp.logical_not(own_first))
        def _():
            send_x(b)

        par_copy(b, 1 - core).wait_recv()

    def rest_from_partner():
        for b in range(1, nb_a):
            from_partner(b)

        @pl.when(jnp.logical_not(own_first))
        def _():
            for m in range(nb_a, 2 * nb_a):
                send_x(m)

    if near:
        @pl.when(jnp.logical_and(pre, t > 0))
        def _():
            for i in range(1, pieces):
                lead_piece(i)
                send_piece(i)

        lead_units(1, min(2, np_))
    from_partner(0)
    if near:
        lead_units(min(2, np_), np_)
    tables = [
        pltpu.make_async_copy(src, dst, sm_sem.at[i])
        for i, (src, dst) in enumerate(((ids_hbm, ids), (live_hbm, live), (slots_hbm, slots)))
    ]
    if not near:
        rest_from_partner()

    def fetch(c, m):
        x_arrival(c, m).wait_recv()
        pass_on(c, m).start()

    def fetched(c, m):
        pass_on(c, m).wait_recv()

    def tell(i, to):
        pl.semaphore_signal(ready.at[i], inc=1, device_id={"tensor": to}, device_id_type=MESH)

    @pl.when(t == 0)
    def _():
        tell(0, right)

    @pl.when(t == T - 1)
    def _():
        tell(1, left)

    def relay():
        @pl.when(jnp.logical_and(t > 0, t < T - 1))
        def _():
            pl.semaphore_wait(ready.at[0], 1)
            tell(0, right)
            pl.semaphore_wait(ready.at[1], 1)
            tell(1, left)

    def all_in():
        @pl.when(t == 0)
        def _():
            pl.semaphore_wait(ready.at[1], 1)

        @pl.when(t == T - 1)
        def _():
            pl.semaphore_wait(ready.at[0], 1)

    def slot_of(k):
        return slots[ids[k]]

    def dn_copy(i):
        to = (a + i) % A
        return pltpu.make_async_remote_copy(
            dn_send.at[to], dn_recv.at[a], sent.at[3], dn_rs.at[0],
            device_id={"adapter": to}, device_id_type=MESH,
        )

    def up_copy(i):
        to = (a + i) % A
        return pltpu.make_async_remote_copy(
            up_send.at[to], up_recv.at[a], sent.at[4], up_rs.at[0],
            device_id={"adapter": to}, device_id_type=MESH,
        )

    def bulk(r, i, recv):
        return pltpu.make_async_remote_copy(
            r, r, sent.at[i], recv, device_id={"adapter": partner}, device_id_type=MESH
        )

    dn_all = bulk(dn_recv.at[pl.ds(0, A - 1)], 3, dn_rs.at[0])
    up_all = bulk(up_recv.at[pl.ds(0, A - 1)], 4, up_rs.at[0])

    def s_dest(b):
        k = a * nb_a + b
        return k // nb_t, k % nb_t

    def col_copy(b):
        return pltpu.make_async_remote_copy(
            s_send.at[b], s_col.at[b, t], col_ss.at[b], col_rs.at[b],
            device_id={"tensor": s_dest(b)[0]}, device_id_type=MESH,
        )

    def s_copy(i, b):
        return pltpu.make_async_remote_copy(
            s_col.at[b], s_recv.at[s_dest(b)[1]], s_ss.at[b], s_rs.at[s_dest(b)[1]],
            device_id={"adapter": (a + i) % A}, device_id_type=MESH,
        )

    def send_adapters():
        for c in tables:
            c.wait()
        dn_load.wait()
        for i in range(A):
            for b in range(nb_a):
                dn_send[i, b] = dn[lax.rem(slot_of(i * nb_a + b), per_dev)]
        dn_recv[a] = dn_send[a]
        for i in range(1, A):
            dn_copy(i).start()
        up_load.wait()
        for b in range(nb_t):
            sl = lax.rem(slot_of(t * nb_t + b), per_dev)
            for i in range(A):
                up_send[i, b] = up[sl, :, i * cols:(i + 1) * cols]
        up_recv[a] = up_send[a]
        for i in range(1, A):
            up_copy(i).start()

    def send_shrunk():
        all_in()
        dn_all.wait_recv()
        for b in range(nb_a):
            k = a * nb_a + b
            mine = dn_recv[lax.div(slot_of(k), per_dev), b]
            s = lax.dot_general(
                mine, tok[k], (((1,), (1,)), ((), ())), preferred_element_type=jnp.float32
            )
            keep = lax.broadcasted_iota(jnp.int32, s.shape, 1) < live[k]
            s_send[b] = jnp.where(keep, s, 0.0).astype(s_send.dtype)
            d, _ = s_dest(b)

            @pl.when(d == t)
            def _():
                s_col[b, t] = s_send[b]

            @pl.when(d != t)
            def _():
                col_copy(b).start()

    def share_shrunk():
        for b in range(nb_a):
            d, kk = s_dest(b)

            @pl.when(d == t)
            def _():
                r = s_col.at[b, pl.ds(0, T - 1)]
                pltpu.make_async_remote_copy(
                    r, r, col_ss.at[b], col_rs.at[b],
                    device_id={"tensor": right}, device_id_type=MESH,
                ).wait_recv()
                for i in range(1, A):
                    s_copy(i, b).start()
                s_recv[kk] = s_col[b]

    def wait_adapters():
        up_all.wait_recv()
        for b in range(nb_t):

            @pl.when((t * nb_t + b) // nb_a != a)
            def _():
                pltpu.make_async_remote_copy(
                    s_recv.at[b], s_recv.at[b], s_ss.at[0], s_rs.at[b],
                    device_id={"adapter": partner}, device_id_type=MESH,
                ).wait_recv()

    remote = [(i, m) for i in range(1, chips) for m in range(2 * nb_a)]
    if not near:
        for i, m in remote:
            fetch((x + i) % chips, m)
        for i, m in remote:
            fetched((x + i) % chips, m)

    units = steps * np_
    if near:
        late = jnp.logical_or(
            jnp.logical_and(t == 0, x == 1), jnp.logical_and(t == T - 1, x == 0)
        )
    lags = (LAG * t, LAG * (T - 1 - t))

    def advance(way, n):
        m = n - lags[way]
        inside = jnp.logical_and(m >= 0, m < units)
        m = jnp.clip(m, 0, units - 1)
        k, p = m // np_, m % np_
        d, h = place(way, k)
        slot = d if way else d - 1
        go = jnp.logical_and(inside, (d < t) if way else (d > t))
        if near:
            go = jnp.logical_and(go, jnp.logical_not(jnp.logical_and(pre, m < np_)))

        @pl.when(go)
        def _():
            mine = base(d * nb_t + h, p)
            fresh = (t == T - 1) if way else (t == 0)

            @pl.when(fresh)
            def _():
                buf[way, slot, h, p] = mine.astype(buf.dtype)

            @pl.when(jnp.logical_not(fresh))
            def _():
                arrival(way, slot, h, p).wait_recv()
                buf[way, slot, h, p] = (
                    mine + buf[way, slot, h, p].astype(jnp.float32)
                ).astype(buf.dtype)

            toward(way, slot, h, p).start()

    def iteration(n, _):
        k, p = n // np_, n % np_
        if near:

            @pl.when(n == min(1, np_))
            def _():
                rest_from_partner()

            @pl.when(jnp.logical_and(p == 0, jnp.logical_and(k >= 1, k <= 2 * nb_a)))
            def _():
                def one(m, _):
                    fetch(1 - x, m)
                    fetched(1 - x, m)
                    return 0

                lo = jnp.where(late, jnp.where(k == 2 * nb_a, 0, k), k - 1)
                lax.fori_loop(lo, k, one, 0)

        @pl.when(n == min(1, steps - 1) * np_)
        def _():
            for c in tables + [dn_load, up_load]:
                c.start()
            relay()

        @pl.when(n == min(2, steps - 1) * np_)
        def _():
            send_adapters()

        @pl.when(n == max(steps - 2, 0) * np_)
        def _():
            send_shrunk()

        loaded = k == 0
        if near:
            loaded = jnp.logical_and(loaded, jnp.logical_not(pre))

        @pl.when(loaded)
        def _():
            @pl.when(p == 0)
            def _():
                for i in range(pieces):
                    w_piece(i).wait()

            @pl.when(p > 0)
            def _():
                w_load(p).wait()

        advance(0, n)
        advance(1, n)
        h = k - (steps - nb_t)

        @pl.when(jnp.logical_and(h >= 0, h < nb_t))
        def _():
            acc[h, p] = base(t * nb_t + h, p)

        return 0

    lax.fori_loop(0, units + LAG * (T - 2), iteration, 0)
    share_shrunk()
    wait_adapters()
    bulk(tok.at[pl.ds(0, nb_a)], 0, par_rs.at[0, 0]).wait_send()
    if chips > 1:
        moved = tok.at[pl.ds(0, (chips - 1) * nb_a)]
        bulk(moved, 1, x_rs.at[0, 0]).wait_send()
        bulk(moved, 2, f_rs.at[0, 0]).wait_send()
    dn_all.wait_send()
    up_all.wait_send()
    for b in range(nb_a):
        d, _ = s_dest(b)

        @pl.when(d == t)
        def _():
            r = dn_send.at[pl.ds(0, A - 1), 0, :, pl.ds(0, T * BLOCK)]
            pltpu.make_async_remote_copy(
                r, r, s_ss.at[b], s_rs.at[0],
                device_id={"adapter": partner}, device_id_type=MESH,
            ).wait_send()

        @pl.when(d != t)
        def _():
            col_copy(b).wait_send()

    def last(n, _):
        h, p = n // np_, n % np_
        own = lax.div(slot_of(t * nb_t + h), per_dev)
        u = up_recv[own, h, :, pl.ds(pl.multiple_of(p * cp, cp), cp)]
        lhs = s_recv[h].reshape(T * s_recv.shape[2], BLOCK)
        acc[h, p] = acc[h, p] + SCALE * lax.dot_general(
            lhs, jnp.concatenate([u] * T, axis=0), (((0,), (0,)), ((), ())),
            preferred_element_type=jnp.float32,
        )

        @pl.when(t > 0)
        def _():
            slot = jnp.maximum(t - 1, 0)
            arrival(0, slot, h, p).wait_recv()
            acc[h, p] = acc[h, p] + buf[0, slot, h, p].astype(jnp.float32)

        @pl.when(t < T - 1)
        def _():
            slot = jnp.minimum(t, T - 2)
            arrival(1, slot, h, p).wait_recv()
            acc[h, p] = acc[h, p] + buf[1, slot, h, p].astype(jnp.float32)

        out_ref[
            pl.ds(pl.multiple_of(h * BLOCK, BLOCK), BLOCK), pl.ds(pl.multiple_of(p * cp, cp), cp)
        ] = acc[h, p].astype(out_ref.dtype)
        return 0

    lax.fori_loop(0, nb_t * np_, last, 0)

    def drain(way, count):
        r = buf.at[way, pl.ds(0, count)]
        pltpu.make_async_remote_copy(
            r, r, fl_ss.at[way], fl_rs.at[0, 0, 0],
            device_id={"tensor": left if way else right}, device_id_type=MESH,
        ).wait_send()

    for i in range(T):

        @pl.when(t == i)
        def _():
            if i < T - 1:
                drain(0, T - 1 - i)
            if i > 0:
                drain(1, i)


def on_device(tokens, query_weight, down, up, ids, live, slots):
    A, T = lax.axis_size("adapter"), lax.axis_size("tensor")
    rows_a, feat = tokens.shape
    cols = query_weight.shape[1]
    rank = down.shape[1]
    rows_d = rows_a * A // T
    cp = min(512, cols)
    np_ = cols // cp
    nb_a, nb_t = rows_a // BLOCK, rows_d // BLOCK
    chips = A // 2
    bf, f32 = jnp.bfloat16, jnp.float32
    dma = pltpu.SemaphoreType.DMA
    hbm = pl.BlockSpec(memory_space=pl.ANY)
    return pl.pallas_call(
        functools.partial(kernel, A, T),
        out_shape=pltpu.VMEM((rows_d, cols), bf),
        in_specs=[hbm] * 7,
        out_specs=pl.BlockSpec(memory_space=pltpu.VMEM),
        scratch_shapes=[
            pltpu.SMEM(ids.shape, ids.dtype),
            pltpu.SMEM(live.shape, live.dtype),
            pltpu.SMEM(slots.shape, slots.dtype),
            pltpu.VMEM((A * nb_a, BLOCK, feat), bf),
            pltpu.VMEM((np_, feat, cp), bf),
            pltpu.VMEM(down.shape, bf),
            pltpu.VMEM(up.shape, bf),
            pltpu.VMEM((2, T - 1, nb_t, np_, BLOCK, cp), bf),
            pltpu.VMEM((nb_t, np_, BLOCK, cp), f32),
            pltpu.VMEM((A, nb_a, rank, feat), bf),
            pltpu.VMEM((A, nb_a, rank, feat), bf),
            pltpu.VMEM((A, nb_t, rank, cols), bf),
            pltpu.VMEM((A, nb_t, rank, cols), bf),
            pltpu.VMEM((nb_a, rank, BLOCK), bf),
            pltpu.VMEM((nb_a, T, rank, BLOCK), bf),
            pltpu.VMEM((nb_t, T, rank, BLOCK), bf),
            dma((3,)), dma((max(nb_a, 2),)), dma((np_ + 1,)), dma((5,)),
            dma((nb_a, 2)), dma((max(chips - 1, 1), 2 * nb_a)), dma((max(chips - 1, 1), 2 * nb_a)),
            dma((1,)), dma((1,)),
            dma((nb_a,)), dma((nb_a,)), dma((nb_a,)), dma((nb_t,)),
            dma((2,)), dma((T + 1, nb_t, np_)),
            pltpu.SemaphoreType.REGULAR((2,)),
        ],
        compiler_params=pltpu.CompilerParams(
            collective_id=0, has_side_effects=True, vmem_limit_bytes=60 * 1024 * 1024
        ),
    )(ids, live, slots, tokens, query_weight, down, up)


def solution(mesh):
    placed = (
        P(("groups", "adapter"), "tensor"),
        P("tensor", "adapter"),
        P("adapter", None, "tensor"),
        P("adapter", None, None),
        P("groups"),
        P("groups"),
        P("groups"),
    )
    return jax.shard_map(
        on_device,
        mesh=mesh,
        in_specs=placed,
        out_specs=P(("groups", "tensor"), "adapter"),
        check_vma=False,
    )
```

```python
import functools

import jax
import jax.numpy as jnp
from jax import lax
from jax.experimental import pallas as pl
from jax.experimental.pallas import tpu as pltpu
from jax.sharding import PartitionSpec as P

BLOCK = 128
SCALE = 2.0
MESH = pl.DeviceIdType.MESH
LAG = 4
GROUP = 2


def kernel(
    A, T,
    ids_hbm, live_hbm, slots_hbm, tok_hbm, w_hbm, dn_hbm, up_hbm, out_ref,
    ids, live, slots, tok, w, dn, up, buf, acc, dn_send, dn_recv, up_send, up_recv,
    s_send, s_col, s_recv,
    sm_sem, ld_sem, w_sem, sent, par_rs, x_rs, f_rs, dn_rs, up_rs,
    col_ss, col_rs, s_ss, s_rs, fl_ss, fl_rs, ready,
):
    a = lax.axis_index("adapter")
    t = lax.axis_index("tensor")
    chips = A // 2
    x, core = a // 2, a % 2
    partner = 2 * x + 1 - core
    nb = tok.shape[0]
    nb_a, nb_t = nb // A, nb // T
    half = BLOCK // 2
    per_dev = dn_hbm.shape[0]
    np_, _, cp = w.shape
    cols = np_ * cp
    group = GROUP if np_ % GROUP == 0 else 1
    steps = (T - 1) * nb_t
    near = chips == 2 and nb_a == nb_t

    def tok_load(b):
        return pltpu.make_async_copy(
            tok_hbm.at[pl.ds(b * BLOCK, BLOCK)], tok.at[a * nb_a + b], ld_sem.at[b]
        )

    piece = cp // 2 if cp % 256 == 0 else cp
    pieces = cp // piece

    def w_piece(i):
        c = pl.ds(i * piece, piece)
        return pltpu.make_async_copy(
            w_hbm.at[:, c], w.at[0, :, c], w_sem.at[np_ if i else 0]
        )

    def w_load(p):
        c = pl.ds(pl.multiple_of(p * cp, cp), cp)
        return pltpu.make_async_copy(w_hbm.at[:, c], w.at[p], w_sem.at[p])

    dn_load = pltpu.make_async_copy(dn_hbm, dn, ld_sem.at[0])
    up_load = pltpu.make_async_copy(up_hbm, up, ld_sem.at[1])

    tok_load(0).start()
    w_piece(0).start()

    barrier = pltpu.get_barrier_semaphore()

    def greet(**to):
        pl.semaphore_signal(barrier, inc=1, device_id=to, device_id_type=MESH)

    @pl.when(t > 0)
    def _():
        greet(tensor=t - 1)

    @pl.when(t < T - 1)
    def _():
        greet(tensor=t + 1)

    for i in range(1, A):
        greet(adapter=(a + i) % A)

    if near:
        lead_r = jnp.where(a >= 1, a, 1)
        lead_l = jnp.where(a <= T - 2, a, T - 2)
        first_r = (T - 1 - lead_r) * nb_t
        first_l = lead_l * nb_t
        pre = jnp.logical_or(
            jnp.logical_and(t == 0, a >= 1), jnp.logical_and(t == T - 1, a <= T - 2)
        )
    else:
        first_r = first_l = 0

    def place(way, k):
        first = first_l if way else first_r
        m = jnp.where(k - 1 < first, k - 1, k)
        m = jnp.where(k == 0, first, m)
        d = m // nb_t
        return (d if way else T - 1 - d), m % nb_t

    def row(way, to, slot):
        return jnp.where(way == 0, slot + 1, jnp.where(slot == to, T, slot))

    def flow(way, to, slot, h, p):
        return pltpu.make_async_remote_copy(
            buf.at[way, slot, h, p], buf.at[way, slot, h, p],
            fl_ss.at[way], fl_rs.at[row(way, to, slot), h, p // group],
            device_id={"tensor": to}, device_id_type=MESH,
        )

    right, left = (t + 1) % T, (t + T - 1) % T

    def toward(way, slot, h, p):
        return flow(way, left if way else right, slot, h, p)

    def arrival(way, slot, h, p):
        r = buf.at[way, slot, h, pl.ds(p, group)]
        return pltpu.make_async_remote_copy(
            r, r, fl_ss.at[way], fl_rs.at[row(way, t, slot), h, p // group],
            device_id={"tensor": left if way else right}, device_id_type=MESH,
        )

    def base(q, p):
        return jnp.dot(tok[q], w[p], preferred_element_type=jnp.float32)

    if near:
        pre_way = jnp.where(t == 0, 0, 1)
        pre_slot = jnp.where(t == 0, jnp.maximum(a - 1, 0), jnp.minimum(a, T - 2))
        pre_to = jnp.where(t == 0, 1, T - 2)

    def lead_unit(p):
        w_load(p).wait()
        buf[pre_way, pre_slot, 0, p] = base(a * nb_a, p).astype(buf.dtype)

    def lead_piece(i):
        w_piece(i).wait()
        c = slice(i * piece, (i + 1) * piece)
        buf[pre_way, pre_slot, 0, 0, :, c] = jnp.dot(
            tok[a * nb_a], w[0, :, c], preferred_element_type=jnp.float32
        ).astype(buf.dtype)

    def send_piece(i):
        r = buf.at[pre_way, pre_slot, 0, 0, :, pl.ds(i * piece, piece)]
        pltpu.make_async_remote_copy(
            r, r, fl_ss.at[pre_way], fl_rs.at[row(pre_way, pre_to, pre_slot), 0, 0],
            device_id={"tensor": pre_to}, device_id_type=MESH,
        ).start()

    for i in range(1, pieces):
        w_piece(i).start()
    for b in range(1, nb_a):
        tok_load(b).start()
    for p in range(1, min(2, np_)):
        w_load(p).start()
    tok_load(0).wait()
    if near:
        @pl.when(pre)
        def _():
            lead_piece(0)

        @pl.when(jnp.logical_and(pre, t == 0))
        def _():
            for i in range(1, pieces):
                lead_piece(i)

    for p in range(2, np_):
        w_load(p).start()

    ends = jnp.where(t > 0, 1, 0) + jnp.where(t < T - 1, 1, 0)
    pl.semaphore_wait(barrier, A - 1 + ends)

    def par_copy(b, k):
        r = part(a * nb_a + b, k)
        return pltpu.make_async_remote_copy(
            r, r, sent.at[0], par_rs.at[b, k],
            device_id={"adapter": partner}, device_id_type=MESH,
        )

    def lead_core(c):
        return jnp.where(2 * c >= chips, 1, 0)

    def row_block(c, m):
        k = jnp.where(m < nb_a, lead_core(c), 1 - lead_core(c))
        return (2 * c + k) * nb_a + m % nb_a, k

    def part(q, k):
        return tok.at[q, pl.ds(pl.multiple_of(k * half, half), half)]

    def x_copy(i, m):
        r = part(row_block(x, m)[0], core)
        return pltpu.make_async_remote_copy(
            r, r, sent.at[1], x_rs.at[i - 1, m],
            device_id={"adapter": 2 * ((x + i) % chips) + core}, device_id_type=MESH,
        )

    def hop(c):
        return (x - c + chips) % chips - 1

    def x_arrival(c, m):
        r = part(row_block(c, m)[0], core)
        return pltpu.make_async_remote_copy(
            r, r, sent.at[1], x_rs.at[hop(c), m],
            device_id={"adapter": partner}, device_id_type=MESH,
        )

    def pass_on(c, m):
        r = part(row_block(c, m)[0], core)
        return pltpu.make_async_remote_copy(
            r, r, sent.at[2], f_rs.at[hop(c), m],
            device_id={"adapter": partner}, device_id_type=MESH,
        )

    def send_x(m):
        for i in range(1, chips):
            x_copy(i, m).start()

    if near:

        @pl.when(pre)
        def _():
            send_piece(0)

        @pl.when(jnp.logical_and(pre, t == 0))
        def _():
            for i in range(1, pieces):
                send_piece(i)

    for b in range(nb_a):
        if b:
            tok_load(b).wait()
        par_copy(b, 1 - core).start()
        par_copy(b, core).start()

    own_first = lead_core(x) == core

    @pl.when(own_first)
    def _():
        for m in range(nb_a):
            send_x(m)

    def lead_units(lo, hi):
        @pl.when(pre)
        def _():
            def one(p, _):
                lead_unit(p)
                flow(pre_way, pre_to, pre_slot, 0, p).start()
                return 0

            lax.fori_loop(lo, hi, one, 0)

    def from_partner(b):
        par_copy(b, core).wait_recv()

        @pl.when(own_first)
        def _():
            send_x(nb_a + b)

        @pl.when(jnp.logical_not(own_first))
        def _():
            send_x(b)

        par_copy(b, 1 - core).wait_recv()

    def rest_from_partner():
        for b in range(1, nb_a):
            from_partner(b)

        @pl.when(jnp.logical_not(own_first))
        def _():
            for m in range(nb_a, 2 * nb_a):
                send_x(m)

    if near:
        @pl.when(jnp.logical_and(pre, t > 0))
        def _():
            for i in range(1, pieces):
                lead_piece(i)
                send_piece(i)

        lead_units(1, min(2, np_))
    from_partner(0)
    if near:
        lead_units(min(2, np_), np_)
    tables = [
        pltpu.make_async_copy(src, dst, sm_sem.at[i])
        for i, (src, dst) in enumerate(((ids_hbm, ids), (live_hbm, live), (slots_hbm, slots)))
    ]
    if not near:
        rest_from_partner()

    def fetch(c, m):
        x_arrival(c, m).wait_recv()
        pass_on(c, m).start()

    def fetched(c, m):
        pass_on(c, m).wait_recv()

    def tell(i, to):
        pl.semaphore_signal(ready.at[i], inc=1, device_id={"tensor": to}, device_id_type=MESH)

    @pl.when(t == 0)
    def _():
        tell(0, right)

    @pl.when(t == T - 1)
    def _():
        tell(1, left)

    def relay():
        @pl.when(jnp.logical_and(t > 0, t < T - 1))
        def _():
            pl.semaphore_wait(ready.at[0], 1)
            tell(0, right)
            pl.semaphore_wait(ready.at[1], 1)
            tell(1, left)

    def all_in():
        @pl.when(t == 0)
        def _():
            pl.semaphore_wait(ready.at[1], 1)

        @pl.when(t == T - 1)
        def _():
            pl.semaphore_wait(ready.at[0], 1)

    def slot_of(k):
        return slots[ids[k]]

    def dn_copy(i):
        to = (a + i) % A
        return pltpu.make_async_remote_copy(
            dn_send.at[to], dn_recv.at[a], sent.at[3], dn_rs.at[0],
            device_id={"adapter": to}, device_id_type=MESH,
        )

    def up_copy(i):
        to = (a + i) % A
        return pltpu.make_async_remote_copy(
            up_send.at[to], up_recv.at[a], sent.at[4], up_rs.at[0],
            device_id={"adapter": to}, device_id_type=MESH,
        )

    def bulk(r, i, recv):
        return pltpu.make_async_remote_copy(
            r, r, sent.at[i], recv, device_id={"adapter": partner}, device_id_type=MESH
        )

    dn_all = bulk(dn_recv.at[pl.ds(0, A - 1)], 3, dn_rs.at[0])
    up_all = bulk(up_recv.at[pl.ds(0, A - 1)], 4, up_rs.at[0])

    def s_dest(b):
        k = a * nb_a + b
        return k // nb_t, k % nb_t

    def col_copy(b):
        return pltpu.make_async_remote_copy(
            s_send.at[b], s_col.at[b, t], col_ss.at[b], col_rs.at[b],
            device_id={"tensor": s_dest(b)[0]}, device_id_type=MESH,
        )

    def s_copy(i, b):
        return pltpu.make_async_remote_copy(
            s_col.at[b], s_recv.at[s_dest(b)[1]], s_ss.at[b], s_rs.at[s_dest(b)[1]],
            device_id={"adapter": (a + i) % A}, device_id_type=MESH,
        )

    def send_adapters():
        for c in tables:
            c.wait()
        dn_load.wait()
        for i in range(A):
            for b in range(nb_a):
                dn_send[i, b] = dn[lax.rem(slot_of(i * nb_a + b), per_dev)]
        dn_recv[a] = dn_send[a]
        for i in range(1, A):
            dn_copy(i).start()
        up_load.wait()
        for b in range(nb_t):
            sl = lax.rem(slot_of(t * nb_t + b), per_dev)
            for i in range(A):
                up_send[i, b] = up[sl, :, i * cols:(i + 1) * cols]
        up_recv[a] = up_send[a]
        for i in range(1, A):
            up_copy(i).start()

    def send_shrunk():
        all_in()
        dn_all.wait_recv()
        for b in range(nb_a):
            k = a * nb_a + b
            mine = dn_recv[lax.div(slot_of(k), per_dev), b]
            s = lax.dot_general(
                mine, tok[k], (((1,), (1,)), ((), ())), preferred_element_type=jnp.float32
            )
            keep = lax.broadcasted_iota(jnp.int32, s.shape, 1) < live[k]
            s_send[b] = jnp.where(keep, s, 0.0).astype(s_send.dtype)
            d, _ = s_dest(b)

            @pl.when(d == t)
            def _():
                s_col[b, t] = s_send[b]

            @pl.when(d != t)
            def _():
                col_copy(b).start()

    def share_shrunk():
        for b in range(nb_a):
            d, kk = s_dest(b)

            @pl.when(d == t)
            def _():
                r = s_col.at[b, pl.ds(0, T - 1)]
                pltpu.make_async_remote_copy(
                    r, r, col_ss.at[b], col_rs.at[b],
                    device_id={"tensor": right}, device_id_type=MESH,
                ).wait_recv()
                for i in range(1, A):
                    s_copy(i, b).start()
                s_recv[kk] = s_col[b]

    def wait_adapters():
        up_all.wait_recv()
        for b in range(nb_t):

            @pl.when((t * nb_t + b) // nb_a != a)
            def _():
                pltpu.make_async_remote_copy(
                    s_recv.at[b], s_recv.at[b], s_ss.at[0], s_rs.at[b],
                    device_id={"adapter": partner}, device_id_type=MESH,
                ).wait_recv()

    remote = [(i, m) for i in range(1, chips) for m in range(2 * nb_a)]
    if not near:
        for i, m in remote:
            fetch((x + i) % chips, m)
        for i, m in remote:
            fetched((x + i) % chips, m)

    units = steps * np_
    if near:
        late = jnp.logical_or(
            jnp.logical_and(t == 0, x == 1), jnp.logical_and(t == T - 1, x == 0)
        )
    lags = (LAG * t, LAG * (T - 1 - t))

    def advance(way, n):
        m = n - lags[way]
        inside = jnp.logical_and(m >= 0, m < units)
        m = jnp.clip(m, 0, units - 1)
        k, p = m // np_, m % np_
        d, h = place(way, k)
        slot = d if way else d - 1
        go = jnp.logical_and(inside, (d < t) if way else (d > t))
        if near:
            go = jnp.logical_and(go, jnp.logical_not(jnp.logical_and(pre, m < np_)))

        @pl.when(go)
        def _():
            mine = base(d * nb_t + h, p)
            fresh = (t == T - 1) if way else (t == 0)

            @pl.when(fresh)
            def _():
                buf[way, slot, h, p] = mine.astype(buf.dtype)

            @pl.when(jnp.logical_not(fresh))
            def _():
                @pl.when(p % group == 0)
                def _():
                    arrival(way, slot, h, p).wait_recv()

                buf[way, slot, h, p] = (
                    mine + buf[way, slot, h, p].astype(jnp.float32)
                ).astype(buf.dtype)

            toward(way, slot, h, p).start()

    def iteration(n, _):
        k, p = n // np_, n % np_
        if near:

            @pl.when(n == min(1, np_))
            def _():
                rest_from_partner()

            @pl.when(jnp.logical_and(p == 0, jnp.logical_and(k >= 1, k <= 2 * nb_a)))
            def _():
                def one(m, _):
                    fetch(1 - x, m)
                    fetched(1 - x, m)
                    return 0

                lo = jnp.where(late, jnp.where(k == 2 * nb_a, 0, k), k - 1)
                lax.fori_loop(lo, k, one, 0)

        @pl.when(n == min(1, steps - 1) * np_)
        def _():
            for c in tables + [dn_load, up_load]:
                c.start()
            relay()

        @pl.when(n == min(2, steps - 1) * np_)
        def _():
            send_adapters()

        @pl.when(n == max(steps - 2, 0) * np_)
        def _():
            send_shrunk()

        loaded = k == 0
        if near:
            loaded = jnp.logical_and(loaded, jnp.logical_not(pre))

        @pl.when(loaded)
        def _():
            @pl.when(p == 0)
            def _():
                for i in range(pieces):
                    w_piece(i).wait()

            @pl.when(p > 0)
            def _():
                w_load(p).wait()

        advance(0, n)
        advance(1, n)
        h = k - (steps - nb_t)

        @pl.when(jnp.logical_and(h >= 0, h < nb_t))
        def _():
            acc[h, p] = base(t * nb_t + h, p)

        return 0

    lax.fori_loop(0, units + LAG * (T - 2), iteration, 0)
    share_shrunk()
    wait_adapters()
    bulk(tok.at[pl.ds(0, nb_a)], 0, par_rs.at[0, 0]).wait_send()
    if chips > 1:
        moved = tok.at[pl.ds(0, (chips - 1) * nb_a)]
        bulk(moved, 1, x_rs.at[0, 0]).wait_send()
        bulk(moved, 2, f_rs.at[0, 0]).wait_send()
    dn_all.wait_send()
    up_all.wait_send()
    for b in range(nb_a):
        d, _ = s_dest(b)

        @pl.when(d == t)
        def _():
            r = dn_send.at[pl.ds(0, A - 1), 0, :, pl.ds(0, T * BLOCK)]
            pltpu.make_async_remote_copy(
                r, r, s_ss.at[b], s_rs.at[0],
                device_id={"adapter": partner}, device_id_type=MESH,
            ).wait_send()

        @pl.when(d != t)
        def _():
            col_copy(b).wait_send()

    def adapters(n, _):
        h, p = n // np_, n % np_
        own = lax.div(slot_of(t * nb_t + h), per_dev)
        u = up_recv[own, h, :, pl.ds(pl.multiple_of(p * cp, cp), cp)]
        lhs = s_recv[h].reshape(T * s_recv.shape[2], BLOCK)
        acc[h, p] = acc[h, p] + SCALE * lax.dot_general(
            lhs, jnp.concatenate([u] * T, axis=0), (((0,), (0,)), ((), ())),
            preferred_element_type=jnp.float32,
        )

        return 0

    lax.fori_loop(0, nb_t * np_, adapters, 0)

    def last(n, _):
        h, p = n // np_, n % np_

        @pl.when(t > 0)
        def _():
            slot = jnp.maximum(t - 1, 0)
            @pl.when(p % group == 0)
            def _():
                arrival(0, slot, h, p).wait_recv()

            acc[h, p] = acc[h, p] + buf[0, slot, h, p].astype(jnp.float32)

        @pl.when(t < T - 1)
        def _():
            slot = jnp.minimum(t, T - 2)
            @pl.when(p % group == 0)
            def _():
                arrival(1, slot, h, p).wait_recv()

            acc[h, p] = acc[h, p] + buf[1, slot, h, p].astype(jnp.float32)

        out_ref[
            pl.ds(pl.multiple_of(h * BLOCK, BLOCK), BLOCK), pl.ds(pl.multiple_of(p * cp, cp), cp)
        ] = acc[h, p].astype(out_ref.dtype)
        return 0

    lax.fori_loop(0, nb_t * np_, last, 0)

    def drain(way, count):
        r = buf.at[way, pl.ds(0, count)]
        pltpu.make_async_remote_copy(
            r, r, fl_ss.at[way], fl_rs.at[0, 0, 0],
            device_id={"tensor": left if way else right}, device_id_type=MESH,
        ).wait_send()

    for i in range(T):

        @pl.when(t == i)
        def _():
            if i < T - 1:
                drain(0, T - 1 - i)
            if i > 0:
                drain(1, i)


def on_device(tokens, query_weight, down, up, ids, live, slots):
    A, T = lax.axis_size("adapter"), lax.axis_size("tensor")
    rows_a, feat = tokens.shape
    cols = query_weight.shape[1]
    rank = down.shape[1]
    rows_d = rows_a * A // T
    cp = min(512, cols)
    np_ = cols // cp
    nb_a, nb_t = rows_a // BLOCK, rows_d // BLOCK
    chips = A // 2
    bf, f32 = jnp.bfloat16, jnp.float32
    dma = pltpu.SemaphoreType.DMA
    hbm = pl.BlockSpec(memory_space=pl.ANY)
    return pl.pallas_call(
        functools.partial(kernel, A, T),
        out_shape=pltpu.VMEM((rows_d, cols), bf),
        in_specs=[hbm] * 7,
        out_specs=pl.BlockSpec(memory_space=pltpu.VMEM),
        scratch_shapes=[
            pltpu.SMEM(ids.shape, ids.dtype),
            pltpu.SMEM(live.shape, live.dtype),
            pltpu.SMEM(slots.shape, slots.dtype),
            pltpu.VMEM((A * nb_a, BLOCK, feat), bf),
            pltpu.VMEM((np_, feat, cp), bf),
            pltpu.VMEM(down.shape, bf),
            pltpu.VMEM(up.shape, bf),
            pltpu.VMEM((2, T - 1, nb_t, np_, BLOCK, cp), bf),
            pltpu.VMEM((nb_t, np_, BLOCK, cp), f32),
            pltpu.VMEM((A, nb_a, rank, feat), bf),
            pltpu.VMEM((A, nb_a, rank, feat), bf),
            pltpu.VMEM((A, nb_t, rank, cols), bf),
            pltpu.VMEM((A, nb_t, rank, cols), bf),
            pltpu.VMEM((nb_a, rank, BLOCK), bf),
            pltpu.VMEM((nb_a, T, rank, BLOCK), bf),
            pltpu.VMEM((nb_t, T, rank, BLOCK), bf),
            dma((3,)), dma((max(nb_a, 2),)), dma((np_ + 1,)), dma((5,)),
            dma((nb_a, 2)), dma((max(chips - 1, 1), 2 * nb_a)), dma((max(chips - 1, 1), 2 * nb_a)),
            dma((1,)), dma((1,)),
            dma((nb_a,)), dma((nb_a,)), dma((nb_a,)), dma((nb_t,)),
            dma((2,)), dma((T + 1, nb_t, np_ // GROUP if np_ % GROUP == 0 else np_)),
            pltpu.SemaphoreType.REGULAR((2,)),
        ],
        compiler_params=pltpu.CompilerParams(
            collective_id=0, has_side_effects=True, vmem_limit_bytes=60 * 1024 * 1024
        ),
    )(ids, live, slots, tokens, query_weight, down, up)


def solution(mesh):
    placed = (
        P(("groups", "adapter"), "tensor"),
        P("tensor", "adapter"),
        P("adapter", None, "tensor"),
        P("adapter", None, None),
        P("groups"),
        P("groups"),
        P("groups"),
    )
    return jax.shard_map(
        on_device,
        mesh=mesh,
        in_specs=placed,
        out_specs=P(("groups", "tensor"), "adapter"),
        check_vma=False,
    )
```

```python
import functools

import jax
import jax.numpy as jnp
from jax import lax
from jax.experimental import pallas as pl
from jax.experimental.pallas import tpu as pltpu
from jax.sharding import PartitionSpec as P

BLOCK = 128
SCALE = 2.0
MESH = pl.DeviceIdType.MESH
LAG = 6
GROUP = 4


def kernel(
    A, T,
    ids_hbm, live_hbm, slots_hbm, tok_hbm, w_hbm, dn_hbm, up_hbm, out_ref,
    ids, live, slots, tok, w, dn, up, buf, acc, dn_send, dn_recv, up_send, up_recv,
    s_send, s_col, s_recv,
    sm_sem, ld_sem, w_sem, sent, par_rs, x_rs, f_rs, dn_rs, up_rs,
    col_ss, col_rs, s_ss, s_rs, fl_ss, fl_rs, ready,
):
    a = lax.axis_index("adapter")
    t = lax.axis_index("tensor")
    chips = A // 2
    x, core = a // 2, a % 2
    partner = 2 * x + 1 - core
    nb = tok.shape[0]
    nb_a, nb_t = nb // A, nb // T
    half = BLOCK // 2
    per_dev = dn_hbm.shape[0]
    np_, _, cp = w.shape
    cols = np_ * cp
    group = GROUP if np_ % GROUP == 0 else 1
    steps = (T - 1) * nb_t
    near = chips == 2 and nb_a == nb_t

    def tok_load(b):
        return pltpu.make_async_copy(
            tok_hbm.at[pl.ds(b * BLOCK, BLOCK)], tok.at[a * nb_a + b], ld_sem.at[b]
        )

    piece = cp // 2 if cp % 256 == 0 else cp
    pieces = cp // piece

    def w_piece(i):
        c = pl.ds(i * piece, piece)
        return pltpu.make_async_copy(
            w_hbm.at[:, c], w.at[0, :, c], w_sem.at[np_ if i else 0]
        )

    def w_load(p):
        c = pl.ds(pl.multiple_of(p * cp, cp), cp)
        return pltpu.make_async_copy(w_hbm.at[:, c], w.at[p], w_sem.at[p])

    dn_load = pltpu.make_async_copy(dn_hbm, dn, ld_sem.at[0])
    up_load = pltpu.make_async_copy(up_hbm, up, ld_sem.at[1])

    tok_load(0).start()
    w_piece(0).start()

    barrier = pltpu.get_barrier_semaphore()

    def greet(**to):
        pl.semaphore_signal(barrier, inc=1, device_id=to, device_id_type=MESH)

    @pl.when(t > 0)
    def _():
        greet(tensor=t - 1)

    @pl.when(t < T - 1)
    def _():
        greet(tensor=t + 1)

    for i in range(1, A):
        greet(adapter=(a + i) % A)

    if near:
        lead_r = jnp.where(a >= 1, a, 1)
        lead_l = jnp.where(a <= T - 2, a, T - 2)
        first_r = (T - 1 - lead_r) * nb_t
        first_l = lead_l * nb_t
        pre = jnp.logical_or(
            jnp.logical_and(t == 0, a >= 1), jnp.logical_and(t == T - 1, a <= T - 2)
        )
    else:
        first_r = first_l = 0

    def place(way, k):
        first = first_l if way else first_r
        m = jnp.where(k - 1 < first, k - 1, k)
        m = jnp.where(k == 0, first, m)
        d = m // nb_t
        return (d if way else T - 1 - d), m % nb_t

    def row(way, to, slot):
        return jnp.where(way == 0, slot + 1, jnp.where(slot == to, T, slot))

    def flow(way, to, slot, h, p):
        return pltpu.make_async_remote_copy(
            buf.at[way, slot, h, p], buf.at[way, slot, h, p],
            fl_ss.at[way], fl_rs.at[row(way, to, slot), h, p // group],
            device_id={"tensor": to}, device_id_type=MESH,
        )

    right, left = (t + 1) % T, (t + T - 1) % T

    def toward(way, slot, h, p):
        return flow(way, left if way else right, slot, h, p)

    def arrival(way, slot, h, p):
        r = buf.at[way, slot, h, pl.ds(p, group)]
        return pltpu.make_async_remote_copy(
            r, r, fl_ss.at[way], fl_rs.at[row(way, t, slot), h, p // group],
            device_id={"tensor": left if way else right}, device_id_type=MESH,
        )

    def base(q, p):
        return jnp.dot(tok[q], w[p], preferred_element_type=jnp.float32)

    if near:
        pre_way = jnp.where(t == 0, 0, 1)
        pre_slot = jnp.where(t == 0, jnp.maximum(a - 1, 0), jnp.minimum(a, T - 2))
        pre_to = jnp.where(t == 0, 1, T - 2)

    def lead_unit(p):
        w_load(p).wait()
        buf[pre_way, pre_slot, 0, p] = base(a * nb_a, p).astype(buf.dtype)

    def lead_piece(i):
        w_piece(i).wait()
        c = slice(i * piece, (i + 1) * piece)
        buf[pre_way, pre_slot, 0, 0, :, c] = jnp.dot(
            tok[a * nb_a], w[0, :, c], preferred_element_type=jnp.float32
        ).astype(buf.dtype)

    def send_piece(i):
        r = buf.at[pre_way, pre_slot, 0, 0, :, pl.ds(i * piece, piece)]
        pltpu.make_async_remote_copy(
            r, r, fl_ss.at[pre_way], fl_rs.at[row(pre_way, pre_to, pre_slot), 0, 0],
            device_id={"tensor": pre_to}, device_id_type=MESH,
        ).start()

    for i in range(1, pieces):
        w_piece(i).start()
    for b in range(1, nb_a):
        tok_load(b).start()
    for p in range(1, min(2, np_)):
        w_load(p).start()
    tok_load(0).wait()
    if near:
        @pl.when(pre)
        def _():
            lead_piece(0)

        @pl.when(jnp.logical_and(pre, t == 0))
        def _():
            for i in range(1, pieces):
                lead_piece(i)

    for p in range(2, np_):
        w_load(p).start()

    ends = jnp.where(t > 0, 1, 0) + jnp.where(t < T - 1, 1, 0)
    pl.semaphore_wait(barrier, A - 1 + ends)

    def par_copy(b, k):
        r = part(a * nb_a + b, k)
        return pltpu.make_async_remote_copy(
            r, r, sent.at[0], par_rs.at[b, k],
            device_id={"adapter": partner}, device_id_type=MESH,
        )

    def lead_core(c):
        return jnp.where(2 * c >= chips, 1, 0)

    def row_block(c, m):
        k = jnp.where(m < nb_a, lead_core(c), 1 - lead_core(c))
        return (2 * c + k) * nb_a + m % nb_a, k

    def part(q, k):
        return tok.at[q, pl.ds(pl.multiple_of(k * half, half), half)]

    def x_copy(i, m):
        r = part(row_block(x, m)[0], core)
        return pltpu.make_async_remote_copy(
            r, r, sent.at[1], x_rs.at[i - 1, m],
            device_id={"adapter": 2 * ((x + i) % chips) + core}, device_id_type=MESH,
        )

    def hop(c):
        return (x - c + chips) % chips - 1

    def x_arrival(c, m):
        r = part(row_block(c, m)[0], core)
        return pltpu.make_async_remote_copy(
            r, r, sent.at[1], x_rs.at[hop(c), m],
            device_id={"adapter": partner}, device_id_type=MESH,
        )

    def pass_on(c, m):
        r = part(row_block(c, m)[0], core)
        return pltpu.make_async_remote_copy(
            r, r, sent.at[2], f_rs.at[hop(c), m],
            device_id={"adapter": partner}, device_id_type=MESH,
        )

    def send_x(m):
        for i in range(1, chips):
            x_copy(i, m).start()

    if near:

        @pl.when(pre)
        def _():
            send_piece(0)

        @pl.when(jnp.logical_and(pre, t == 0))
        def _():
            for i in range(1, pieces):
                send_piece(i)

    for b in range(nb_a):
        if b:
            tok_load(b).wait()
        par_copy(b, 1 - core).start()
        par_copy(b, core).start()

    own_first = lead_core(x) == core

    @pl.when(own_first)
    def _():
        for m in range(nb_a):
            send_x(m)

    def lead_units(lo, hi):
        @pl.when(pre)
        def _():
            def one(p, _):
                lead_unit(p)
                flow(pre_way, pre_to, pre_slot, 0, p).start()
                return 0

            lax.fori_loop(lo, hi, one, 0)

    def from_partner(b):
        par_copy(b, core).wait_recv()

        @pl.when(own_first)
        def _():
            send_x(nb_a + b)

        @pl.when(jnp.logical_not(own_first))
        def _():
            send_x(b)

        par_copy(b, 1 - core).wait_recv()

    def rest_from_partner():
        for b in range(1, nb_a):
            from_partner(b)

        @pl.when(jnp.logical_not(own_first))
        def _():
            for m in range(nb_a, 2 * nb_a):
                send_x(m)

    if near:
        @pl.when(jnp.logical_and(pre, t > 0))
        def _():
            for i in range(1, pieces):
                lead_piece(i)
                send_piece(i)

        lead_units(1, min(2, np_))
    from_partner(0)
    if near:
        lead_units(min(2, np_), np_)
    tables = [
        pltpu.make_async_copy(src, dst, sm_sem.at[i])
        for i, (src, dst) in enumerate(((ids_hbm, ids), (live_hbm, live), (slots_hbm, slots)))
    ]
    if not near:
        rest_from_partner()

    def fetch(c, m):
        x_arrival(c, m).wait_recv()
        pass_on(c, m).start()

    def fetched(c, m):
        pass_on(c, m).wait_recv()

    def tell(i, to):
        pl.semaphore_signal(ready.at[i], inc=1, device_id={"tensor": to}, device_id_type=MESH)

    @pl.when(t == 0)
    def _():
        tell(0, right)

    @pl.when(t == T - 1)
    def _():
        tell(1, left)

    def relay():
        @pl.when(jnp.logical_and(t > 0, t < T - 1))
        def _():
            pl.semaphore_wait(ready.at[0], 1)
            tell(0, right)
            pl.semaphore_wait(ready.at[1], 1)
            tell(1, left)

    def all_in():
        @pl.when(t == 0)
        def _():
            pl.semaphore_wait(ready.at[1], 1)

        @pl.when(t == T - 1)
        def _():
            pl.semaphore_wait(ready.at[0], 1)

    def slot_of(k):
        return slots[ids[k]]

    def dn_copy(i):
        to = (a + i) % A
        return pltpu.make_async_remote_copy(
            dn_send.at[to], dn_recv.at[a], sent.at[3], dn_rs.at[0],
            device_id={"adapter": to}, device_id_type=MESH,
        )

    def up_copy(i):
        to = (a + i) % A
        return pltpu.make_async_remote_copy(
            up_send.at[to], up_recv.at[a], sent.at[4], up_rs.at[0],
            device_id={"adapter": to}, device_id_type=MESH,
        )

    def bulk(r, i, recv):
        return pltpu.make_async_remote_copy(
            r, r, sent.at[i], recv, device_id={"adapter": partner}, device_id_type=MESH
        )

    dn_all = bulk(dn_recv.at[pl.ds(0, A - 1)], 3, dn_rs.at[0])
    up_all = bulk(up_recv.at[pl.ds(0, A - 1)], 4, up_rs.at[0])

    def s_dest(b):
        k = a * nb_a + b
        return k // nb_t, k % nb_t

    def col_copy(b):
        return pltpu.make_async_remote_copy(
            s_send.at[b], s_col.at[b, t], col_ss.at[b], col_rs.at[b],
            device_id={"tensor": s_dest(b)[0]}, device_id_type=MESH,
        )

    def s_copy(i, b):
        return pltpu.make_async_remote_copy(
            s_col.at[b], s_recv.at[s_dest(b)[1]], s_ss.at[b], s_rs.at[s_dest(b)[1]],
            device_id={"adapter": (a + i) % A}, device_id_type=MESH,
        )

    def send_adapters():
        for c in tables:
            c.wait()
        dn_load.wait()
        for i in range(A):
            for b in range(nb_a):
                dn_send[i, b] = dn[lax.rem(slot_of(i * nb_a + b), per_dev)]
        dn_recv[a] = dn_send[a]
        for i in range(1, A):
            dn_copy(i).start()
        up_load.wait()
        for b in range(nb_t):
            sl = lax.rem(slot_of(t * nb_t + b), per_dev)
            for i in range(A):
                up_send[i, b] = up[sl, :, i * cols:(i + 1) * cols]
        up_recv[a] = up_send[a]
        for i in range(1, A):
            up_copy(i).start()

    def send_shrunk():
        all_in()
        dn_all.wait_recv()
        for b in range(nb_a):
            k = a * nb_a + b
            mine = dn_recv[lax.div(slot_of(k), per_dev), b]
            s = lax.dot_general(
                mine, tok[k], (((1,), (1,)), ((), ())), preferred_element_type=jnp.float32
            )
            keep = lax.broadcasted_iota(jnp.int32, s.shape, 1) < live[k]
            s_send[b] = jnp.where(keep, s, 0.0).astype(s_send.dtype)
            d, _ = s_dest(b)

            @pl.when(d == t)
            def _():
                s_col[b, t] = s_send[b]

            @pl.when(d != t)
            def _():
                col_copy(b).start()

    def share_shrunk():
        for b in range(nb_a):
            d, kk = s_dest(b)

            @pl.when(d == t)
            def _():
                r = s_col.at[b, pl.ds(0, T - 1)]
                pltpu.make_async_remote_copy(
                    r, r, col_ss.at[b], col_rs.at[b],
                    device_id={"tensor": right}, device_id_type=MESH,
                ).wait_recv()
                for i in range(1, A):
                    s_copy(i, b).start()
                s_recv[kk] = s_col[b]

    def wait_adapters():
        up_all.wait_recv()
        for b in range(nb_t):

            @pl.when((t * nb_t + b) // nb_a != a)
            def _():
                pltpu.make_async_remote_copy(
                    s_recv.at[b], s_recv.at[b], s_ss.at[0], s_rs.at[b],
                    device_id={"adapter": partner}, device_id_type=MESH,
                ).wait_recv()

    remote = [(i, m) for i in range(1, chips) for m in range(2 * nb_a)]
    if not near:
        for i, m in remote:
            fetch((x + i) % chips, m)
        for i, m in remote:
            fetched((x + i) % chips, m)

    units = steps * np_
    if near:
        late = jnp.logical_or(
            jnp.logical_and(t == 0, x == 1), jnp.logical_and(t == T - 1, x == 0)
        )
    lags = (LAG * t, LAG * (T - 1 - t))

    def advance(way, n):
        m = n - lags[way]
        inside = jnp.logical_and(m >= 0, m < units)
        m = jnp.clip(m, 0, units - 1)
        k, p = m // np_, m % np_
        d, h = place(way, k)
        slot = d if way else d - 1
        go = jnp.logical_and(inside, (d < t) if way else (d > t))
        if near:
            go = jnp.logical_and(go, jnp.logical_not(jnp.logical_and(pre, m < np_)))

        @pl.when(go)
        def _():
            mine = base(d * nb_t + h, p)
            fresh = (t == T - 1) if way else (t == 0)

            @pl.when(fresh)
            def _():
                buf[way, slot, h, p] = mine.astype(buf.dtype)

            @pl.when(jnp.logical_not(fresh))
            def _():
                @pl.when(p % group == 0)
                def _():
                    arrival(way, slot, h, p).wait_recv()

                buf[way, slot, h, p] = (
                    mine + buf[way, slot, h, p].astype(jnp.float32)
                ).astype(buf.dtype)

            toward(way, slot, h, p).start()

    def iteration(n, _):
        k, p = n // np_, n % np_
        if near:

            @pl.when(n == min(1, np_))
            def _():
                rest_from_partner()

            @pl.when(jnp.logical_and(p == 0, jnp.logical_and(k >= 1, k <= 2 * nb_a)))
            def _():
                def one(m, _):
                    fetch(1 - x, m)
                    fetched(1 - x, m)
                    return 0

                lo = jnp.where(late, jnp.where(k == 2 * nb_a, 0, k), k - 1)
                lax.fori_loop(lo, k, one, 0)

        @pl.when(n == min(1, steps - 1) * np_)
        def _():
            for c in tables + [dn_load, up_load]:
                c.start()
            relay()

        @pl.when(n == min(2, steps - 1) * np_)
        def _():
            send_adapters()

        @pl.when(n == max(steps - 2, 0) * np_)
        def _():
            send_shrunk()

        loaded = k == 0
        if near:
            loaded = jnp.logical_and(loaded, jnp.logical_not(pre))

        @pl.when(loaded)
        def _():
            @pl.when(p == 0)
            def _():
                for i in range(pieces):
                    w_piece(i).wait()

            @pl.when(p > 0)
            def _():
                w_load(p).wait()

        advance(0, n)
        advance(1, n)
        h = k - (steps - nb_t)

        @pl.when(jnp.logical_and(h >= 0, h < nb_t))
        def _():
            acc[h, p] = base(t * nb_t + h, p)

        return 0

    lax.fori_loop(0, units + LAG * (T - 2), iteration, 0)
    share_shrunk()
    wait_adapters()
    bulk(tok.at[pl.ds(0, nb_a)], 0, par_rs.at[0, 0]).wait_send()
    if chips > 1:
        moved = tok.at[pl.ds(0, (chips - 1) * nb_a)]
        bulk(moved, 1, x_rs.at[0, 0]).wait_send()
        bulk(moved, 2, f_rs.at[0, 0]).wait_send()
    dn_all.wait_send()
    up_all.wait_send()
    for b in range(nb_a):
        d, _ = s_dest(b)

        @pl.when(d == t)
        def _():
            r = dn_send.at[pl.ds(0, A - 1), 0, :, pl.ds(0, T * BLOCK)]
            pltpu.make_async_remote_copy(
                r, r, s_ss.at[b], s_rs.at[0],
                device_id={"adapter": partner}, device_id_type=MESH,
            ).wait_send()

        @pl.when(d != t)
        def _():
            col_copy(b).wait_send()

    def adapters(n, _):
        h, p = n // np_, n % np_
        own = lax.div(slot_of(t * nb_t + h), per_dev)
        u = up_recv[own, h, :, pl.ds(pl.multiple_of(p * cp, cp), cp)]
        lhs = s_recv[h].reshape(T * s_recv.shape[2], BLOCK)
        acc[h, p] = acc[h, p] + SCALE * lax.dot_general(
            lhs, jnp.concatenate([u] * T, axis=0), (((0,), (0,)), ((), ())),
            preferred_element_type=jnp.float32,
        )

        return 0

    lax.fori_loop(0, nb_t * np_, adapters, 0)

    def last(n, _):
        h, p = n // np_, n % np_

        @pl.when(t > 0)
        def _():
            slot = jnp.maximum(t - 1, 0)
            @pl.when(p % group == 0)
            def _():
                arrival(0, slot, h, p).wait_recv()

            acc[h, p] = acc[h, p] + buf[0, slot, h, p].astype(jnp.float32)

        @pl.when(t < T - 1)
        def _():
            slot = jnp.minimum(t, T - 2)
            @pl.when(p % group == 0)
            def _():
                arrival(1, slot, h, p).wait_recv()

            acc[h, p] = acc[h, p] + buf[1, slot, h, p].astype(jnp.float32)

        out_ref[
            pl.ds(pl.multiple_of(h * BLOCK, BLOCK), BLOCK), pl.ds(pl.multiple_of(p * cp, cp), cp)
        ] = acc[h, p].astype(out_ref.dtype)
        return 0

    lax.fori_loop(0, nb_t * np_, last, 0)

    def drain(way, count):
        r = buf.at[way, pl.ds(0, count)]
        pltpu.make_async_remote_copy(
            r, r, fl_ss.at[way], fl_rs.at[0, 0, 0],
            device_id={"tensor": left if way else right}, device_id_type=MESH,
        ).wait_send()

    for i in range(T):

        @pl.when(t == i)
        def _():
            if i < T - 1:
                drain(0, T - 1 - i)
            if i > 0:
                drain(1, i)


def on_device(tokens, query_weight, down, up, ids, live, slots):
    A, T = lax.axis_size("adapter"), lax.axis_size("tensor")
    rows_a, feat = tokens.shape
    cols = query_weight.shape[1]
    rank = down.shape[1]
    rows_d = rows_a * A // T
    cp = min(512, cols)
    np_ = cols // cp
    nb_a, nb_t = rows_a // BLOCK, rows_d // BLOCK
    chips = A // 2
    bf, f32 = jnp.bfloat16, jnp.float32
    dma = pltpu.SemaphoreType.DMA
    hbm = pl.BlockSpec(memory_space=pl.ANY)
    return pl.pallas_call(
        functools.partial(kernel, A, T),
        out_shape=pltpu.VMEM((rows_d, cols), bf),
        in_specs=[hbm] * 7,
        out_specs=pl.BlockSpec(memory_space=pltpu.VMEM),
        scratch_shapes=[
            pltpu.SMEM(ids.shape, ids.dtype),
            pltpu.SMEM(live.shape, live.dtype),
            pltpu.SMEM(slots.shape, slots.dtype),
            pltpu.VMEM((A * nb_a, BLOCK, feat), bf),
            pltpu.VMEM((np_, feat, cp), bf),
            pltpu.VMEM(down.shape, bf),
            pltpu.VMEM(up.shape, bf),
            pltpu.VMEM((2, T - 1, nb_t, np_, BLOCK, cp), bf),
            pltpu.VMEM((nb_t, np_, BLOCK, cp), f32),
            pltpu.VMEM((A, nb_a, rank, feat), bf),
            pltpu.VMEM((A, nb_a, rank, feat), bf),
            pltpu.VMEM((A, nb_t, rank, cols), bf),
            pltpu.VMEM((A, nb_t, rank, cols), bf),
            pltpu.VMEM((nb_a, rank, BLOCK), bf),
            pltpu.VMEM((nb_a, T, rank, BLOCK), bf),
            pltpu.VMEM((nb_t, T, rank, BLOCK), bf),
            dma((3,)), dma((max(nb_a, 2),)), dma((np_ + 1,)), dma((5,)),
            dma((nb_a, 2)), dma((max(chips - 1, 1), 2 * nb_a)), dma((max(chips - 1, 1), 2 * nb_a)),
            dma((1,)), dma((1,)),
            dma((nb_a,)), dma((nb_a,)), dma((nb_a,)), dma((nb_t,)),
            dma((2,)), dma((T + 1, nb_t, np_ // GROUP if np_ % GROUP == 0 else np_)),
            pltpu.SemaphoreType.REGULAR((2,)),
        ],
        compiler_params=pltpu.CompilerParams(
            collective_id=0, has_side_effects=True, vmem_limit_bytes=60 * 1024 * 1024
        ),
    )(ids, live, slots, tokens, query_weight, down, up)


def solution(mesh):
    placed = (
        P(("groups", "adapter"), "tensor"),
        P("tensor", "adapter"),
        P("adapter", None, "tensor"),
        P("adapter", None, None),
        P("groups"),
        P("groups"),
        P("groups"),
    )
    return jax.shard_map(
        on_device,
        mesh=mesh,
        in_specs=placed,
        out_specs=P(("groups", "tensor"), "adapter"),
        check_vma=False,
    )
```
